256 devices in a mesh: gx: 8 (over x_lo, y), gy: 4 (over x_hi, core), gz: 8 (over z).
Axes of the slice: x: 4 (x_hi: 2, x_lo: 2; x = x_hi * 2 + x_lo), y: 4, z: 8, core: 2. Of those that a mesh axis runs over, the one named last changes fastest.
Arguments:
- offsets: float32 [16, 8, 64, 16, 3], P('gx', 'gy', 'gz'), may hold values from 0.2649 to 2.3351, as said below
- velocities: float32 [16, 8, 64, 16, 3], P('gx', 'gy', 'gz'), may hold values from -6 to 6
- occupied: int32 [16, 8, 64, 16], P('gx', 'gy', 'gz'), may hold values 0 or 1
Outputs:
- positions: float32 [16, 8, 64, 16, 3], P('gx', 'gy', 'gz')
- new_velocities: float32 [16, 8, 64, 16, 3], P('gx', 'gy', 'gz')
- forces: float32 [16, 8, 64, 16, 3], P('gx', 'gy', 'gz')
- capacity_history: float32 [4, 2], replicated
The draws below stay inside these ranges and needn't reach their ends.
Inputs may be any that keep to these rules, and one draw needn't show every extreme that they name: `offsets`: each offset lies within the cell, a jittered body-centred lattice of 16 sites with spacing 1.3 per cell, jitter at most 0.06 in each coordinate.
All inputs are finite; a program needn't handle non-finite values.
Results may differ from the reference program's by a relative error of at most 0.0003.
Values sent between devices are 32-bit elements.
A program may use at most 128 MiB of HBM per device.

```python
import jax
import jax.numpy as jnp
from jax import lax

SLOTS = 16
STEPS = 4
NX = 16
NY = 8
NZ = 64


LATTICE_STEP = 1.3


JITTER = 0.06


def draw_offsets(key, part):
    slot_ids = jnp.arange(SLOTS) % 16
    corner = slot_ids % 8
    corner_bits = jnp.stack([corner // 4, corner // 2 % 2, corner % 2], axis=-1).astype(jnp.float32)
    centred = (slot_ids // 8).astype(jnp.float32)[:, None]
    lattice = LATTICE_STEP * (corner_bits + 0.5 * centred) + 0.325
    shape_all = (NX, NY, NZ, SLOTS, 3)
    jitter = jax.random.uniform(key, shape_all, jnp.float32, -JITTER, JITTER)
    return (lattice + jitter).astype(jnp.float32)


def plant(result, key, smallest, largest):
    longest = result.shape.index(max(result.shape))
    spots = []
    for shift in (0, 1):
        where = [jax.random.randint(jax.random.fold_in(key, axis), (), 0, length) for axis, length in enumerate(result.shape)]
        where[longest] = (where[longest] + shift) % result.shape[longest]
        spots.append(tuple(where))
    return result.at[spots[0]].set(smallest).at[spots[1]].set(largest)


def block_levels(stream_key, dims, pieces, least, largest):
    def one(dim, shards_of):
        heights = jax.random.uniform(jax.random.fold_in(jax.random.fold_in(stream_key, 6), dim), (shards_of,), jnp.float32, least / len(pieces), largest / len(pieces))
        return jnp.repeat(jnp.exp(heights), dims[dim] // shards_of).reshape((-1,) + (1,) * (len(dims) - dim - 1))

    loudness = one(*pieces[0])
    for cut in pieces[1:]:
        loudness = loudness * one(*cut)
    return loudness


def bell_draw(own_key, shape, spread, bound, shards=(), kind=jnp.bfloat16):
    level = block_levels(own_key, shape, shards, -0.22, 0.18) if shards else 1.0
    entries = jax.random.normal(own_key, shape, jnp.float32) * spread * level
    return jnp.minimum(jnp.maximum(entries, -bound), bound).astype(kind)


def setup_inputs(seed: int = 0) -> dict:
    keys = jax.random.split(jax.random.key(seed), 4)
    offsets = draw_offsets(jax.random.fold_in(keys[3], 71), 0)
    velocities = bell_draw(keys[1], (NX, NY, NZ, SLOTS, 3), 1.0, 6.0, ((0, 8), (1, 4), (2, 8)), jnp.float32)
    occupied = plant((jax.random.randint(keys[2], (NX, NY, NZ, SLOTS), 0, 16) < 13).astype(jnp.int32), jax.random.fold_in(keys[2], 1), 0, 1)
    return dict(offsets=offsets, velocities=velocities, occupied=occupied)


CUTOFF = 2.5
CELL_SIDE = 2.6
TIME_STEP = 0.005
BATH_STRENGTH = 0.25
GOAL_WARMTH = 0.8
FORCE_EDGE = 24.0 * (2.0 * CUTOFF ** (-13) - CUTOFF ** (-7))
ENERGY_EDGE = 4.0 * (CUTOFF ** (-12) - CUTOFF ** (-6))
STENCILS = [(along_x, along_y, along_z) for along_x in (-1, 0, 1) for along_y in (-1, 0, 1) for along_z in (-1, 0, 1)]

def pair_terms(own_cells, neighbour, stencil):
    cell_shift = jnp.array(stencil, jnp.float32) * CELL_SIDE
    separation = neighbour[..., None, :, :3] + cell_shift - own_cells[..., :, None, :3]
    squared = lax.optimization_barrier(jnp.sum(separation * separation, axis=-1))
    occupied_pair = own_cells[..., :, None, 3] * neighbour[..., None, :, 3]
    inside = (occupied_pair > 0.5) & (squared < CUTOFF * CUTOFF)
    if stencil == (0, 0, 0):
        slots_count = own_cells.shape[-2]
        inside = inside & jnp.logical_not(jnp.eye(slots_count, dtype=bool))
    guarded = jnp.where(inside, squared, 1.0)
    inverse = 1.0 / guarded
    inverse_six = inverse * inverse * inverse
    radius = jnp.sqrt(guarded)
    strength = 24.0 * (2.0 * inverse_six * inverse_six - inverse_six) * inverse - FORCE_EDGE / radius
    strength = jnp.where(inside, strength, 0.0)
    energy = 4.0 * (inverse_six * inverse_six - inverse_six) - ENERGY_EDGE + (radius - CUTOFF) * FORCE_EDGE
    energy = jnp.where(inside, energy, 0.0)
    pushes = -strength[..., None] * separation
    return (pushes, energy)

def window(padded, stencil, extent):
    return padded[1 + stencil[0]:1 + stencil[0] + extent[0], 1 + stencil[1]:1 + stencil[1] + extent[1], 1 + stencil[2]:1 + stencil[2] + extent[2]]

def full_forces(padded):
    extent = (padded.shape[0] - 2, padded.shape[1] - 2, padded.shape[2] - 2)
    own_cells = window(padded, (0, 0, 0), extent)
    forces = jnp.zeros(own_cells.shape[:-1] + (3,), jnp.float32)
    energy = jnp.zeros((), jnp.float32)
    for stencil in STENCILS:
        pushes, pair_energy = pair_terms(own_cells, window(padded, stencil, extent), stencil)
        forces = forces + lax.optimization_barrier(jnp.sum(pushes, axis=-2))
        energy = energy + jnp.sum(pair_energy)
    return (forces, 0.5 * energy)

def evaluate(position, weight):
    packed = jnp.concatenate([position, weight[..., None]], axis=-1)
    padded = jnp.pad(packed, ((1, 1), (1, 1), (1, 1), (0, 0), (0, 0)), mode='wrap')

    def one_plane(plane_index):
        block = lax.dynamic_slice_in_dim(padded, plane_index, 3, 0)
        return full_forces(block)
    forces, capacity_history = lax.map(one_plane, jnp.arange(NX, dtype=jnp.int32))
    return (forces.reshape(position.shape), jnp.sum(capacity_history))

def reference(offsets, velocities, occupied):
    weight = occupied.astype(jnp.float32)
    velocity = velocities * weight[..., None]
    position = offsets
    slot_total = float(NX * NY * NZ * SLOTS)
    forces, initial_energy = evaluate(position, weight)
    body_tally = jnp.sum(weight)
    records = []
    for step_index in range(STEPS):
        velocity = velocity + 0.5 * TIME_STEP * forces
        position = position + TIME_STEP * velocity
        forces, potential = evaluate(position, weight)
        velocity = velocity + 0.5 * TIME_STEP * forces
        moving_vigor = 0.5 * jnp.sum(velocity * velocity)
        warmth_gauge = 2.0 * moving_vigor / (3.0 * body_tally)
        speed_stretch = jnp.sqrt(1.0 + BATH_STRENGTH * (GOAL_WARMTH / warmth_gauge - 1.0))
        velocity = speed_stretch * velocity
        records.append(jnp.stack([potential, speed_stretch * speed_stretch * moving_vigor]) / slot_total)
    return (position, velocity, forces, jnp.stack(records))
```

```python
import functools
import itertools

import jax
import jax.numpy as jnp
from jax import lax
from jax.experimental import pallas as pl
from jax.experimental.pallas import tpu as pltpu
from jax.sharding import PartitionSpec as P

STEPS = 4
ROUNDS = STEPS + 1
CUTOFF = 2.5
CELL_SIDE = 2.6
TIME_STEP = 0.005
BATH_STRENGTH = 0.25
GOAL_WARMTH = 0.8
FORCE_EDGE = 24.0 * (2.0 * CUTOFF ** (-13) - CUTOFF ** (-7))
ENERGY_EDGE = 4.0 * (CUTOFF ** (-12) - CUTOFF ** (-6))
ENERGY_SHIFT = -ENERGY_EDGE - CUTOFF * FORCE_EDGE
FAR = 1.0e6
MESH = pl.DeviceIdType.MESH
LANES = 128
SLOTS = 16
DEPTH = 8

SIDES = {0: (pl.ds(0, 2), pl.ds(1, 2)), 1: (pl.ds(1, 1), pl.ds(0, 1)), -1: (pl.ds(0, 1), pl.ds(3, 1))}
NEIGHBOURS = sorted(
    (d for d in itertools.product((-1, 0, 1), repeat=3) if d != (0, 0, 0)),
    key=lambda d: -(2 * abs(d[0]) + 2 * abs(d[1]) + abs(d[2])),
)


def lane_take(x, lanes):
    return jnp.take_along_axis(x, lanes, axis=1, mode="promise_in_bounds")


def kernel(
    sizes, o_ref, v_ref, w_ref, oo_ref, vo_ref, fo_ref, hist_ref,
    buf, zsrc, zbuf, red_a, red_b, expand, acc, state, shifted, strip,
    halo_recv, halo_send, z_recv, z_send, a_recv, a_send, b_recv, b_send,
):
    nx, ny, nz = sizes
    gx, gy, gz = (lax.axis_index(a) for a in ("gx", "gy", "gz"))
    high, core = gy // 2, gy % 2
    n_high = ny // 2

    def at(dx, dy, dz):
        return (lax.rem(gx + dx + nx, nx), lax.rem(gy + dy + ny, ny), lax.rem(gz + dz + nz, nz))

    group_a = [
        (gx, high * 2 + lax.rem(core + dc, 2), lax.rem(gz + dz, nz))
        for dz in range(nz) for dc in range(2) if (dz, dc) != (0, 0)
    ]
    me_a = gz * 2 + core
    group_b = [
        (lax.rem(gx + dx, nx), lax.rem(high + dh, n_high) * 2 + core, gz)
        for dx in range(nx) for dh in range(n_high) if (dx, dh) != (0, 0)
    ]
    me_b = gx * n_high + high
    size_a, size_b = nz * 2, nx * n_high

    barrier = pltpu.get_barrier_semaphore()
    peers = [at(*d) for d in NEIGHBOURS] + group_a + group_b
    for peer in peers:
        pl.semaphore_signal(barrier, inc=1, device_id=peer, device_id_type=MESH)

    lane = lax.broadcasted_iota(jnp.int32, (8, LANES), 1)
    row = lax.broadcasted_iota(jnp.int32, (8, LANES), 0)
    slot, cell = lane % SLOTS, lane // SLOTS
    lane1 = lane[:1]

    def flatten(block):
        strip[:, :SLOTS] = block
        spread = lane_take(strip[...], slot)
        return jnp.sum(jnp.where(cell == row, spread, 0.0), axis=0, keepdims=True)

    for k in range(16):
        state[k] = jnp.zeros((8, LANES), jnp.float32)
    POS, VEL, FORCE, BASE, TERM, WEIGHT = 0, 3, 6, 9, 12, 15
    for c in range(4):
        cx, cy = c // 2, c % 2
        state[WEIGHT, c : c + 1, :] = flatten(w_ref[cx, cy].astype(jnp.float32))
        for k in range(3):
            state[BASE + k, c : c + 1, :] = flatten(o_ref[cx, cy, k])
            state[VEL + k, c : c + 1, :] = flatten(v_ref[cx, cy, k])
    for k in range(3):
        state[VEL + k] = state[VEL + k] * state[WEIGHT]
    acc[...] = jnp.zeros_like(acc)
    for r in range(ROUNDS):
        for cx in range(2):
            for cy in range(2):
                buf[r, 1 + cx, 1 + cy] = jnp.zeros((2, 4, LANES), jnp.float32)

    def ship(r):
        here = state[WEIGHT] > 0.5
        base = [jnp.where(here, state[BASE + k], FAR) for k in range(3)]
        term = [state[TERM + k] for k in range(3)]
        for c in range(4):
            for k in range(3):
                buf[r, 1 + c // 2, 1 + c % 2, 0, k : k + 1, :] = base[k][c : c + 1]
                buf[r, 1 + c // 2, 1 + c % 2, 1, k : k + 1, :] = term[k][c : c + 1]
        for end in range(2):
            pick = slot + end * (LANES - SLOTS)
            packed = jnp.zeros((8, LANES), jnp.float32)
            for k in range(3):
                packed = jnp.where(cell == k + 4 * end, lane_take(base[k], pick), packed)
                packed = jnp.where(cell == k + 4 - 4 * end, lane_take(term[k], pick), packed)
            for c in range(4):
                zsrc[r, end, c // 2, c % 2] = packed[c : c + 1]
        for dx, dy, dz in NEIGHBOURS:
            (from_x, to_x), (from_y, to_y) = SIDES[dx], SIDES[dy]
            if dz == 0:
                own_x, own_y = pl.ds(from_x.start + 1, from_x.size), pl.ds(from_y.start + 1, from_y.size)
                pltpu.make_async_remote_copy(
                    src_ref=buf.at[r, own_x, own_y], dst_ref=buf.at[r, to_x, to_y],
                    send_sem=halo_send.at[r], recv_sem=halo_recv.at[r],
                    device_id=at(dx, dy, dz), device_id_type=MESH,
                ).start()
            else:
                end = 0 if dz < 0 else 1
                pltpu.make_async_remote_copy(
                    src_ref=zsrc.at[r, end, from_x, from_y], dst_ref=zbuf.at[r, end, to_x, to_y],
                    send_sem=z_send.at[r], recv_sem=z_recv.at[r],
                    device_id=at(dx, dy, dz), device_id_type=MESH,
                ).start()

    def all_of(ref, sem):
        pltpu.make_async_copy(ref, ref, sem).wait()

    def share(stage, me, group, send_sem, recv_sem, k, value):
        stage[k, me] = value
        for peer in group:
            pltpu.make_async_remote_copy(
                src_ref=stage.at[k, me], dst_ref=stage.at[k, me],
                send_sem=send_sem.at[k], recv_sem=recv_sem.at[k],
                device_id=peer, device_id_type=MESH,
            ).start()

    def collect(stage, size, recv_sem, k):
        all_of(stage.at[k, pl.ds(0, size - 1)], recv_sem.at[k])
        return jnp.sum(stage[k], axis=0)

    def half_sum(value, width):
        while width < LANES:
            value = value + pltpu.roll(value, width, 1)
            width *= 2
        return value

    count = jnp.sum(state[WEIGHT], axis=0, keepdims=True)
    count = count + pltpu.roll(count, 64, 1)
    count = count + pltpu.roll(count, 32, 1)

    pl.semaphore_wait(barrier, len(peers))
    ship(0)

    def one_round(r, stretch):
        wide = jnp.broadcast_to(stretch, (8, LANES))
        half_step = jnp.where(r == 0, 0.0, 0.5 * TIME_STEP)
        here = state[WEIGHT] > 0.5
        position, velocity = [], []
        for k in range(3):
            position.append(state[BASE + k] + wide * state[TERM + k])
            velocity.append(wide * state[VEL + k] + (0.5 * TIME_STEP) * state[FORCE + k])
            state[POS + k] = position[k]
            for dz in (-1, 0, 1):
                moved = pltpu.roll(position[k], (SLOTS * dz) % LANES, 1) if dz else position[k]
                shifted[dz + 1, k] = moved - CELL_SIDE * dz if k == 2 else moved

        all_of(buf.at[r, pl.ds(0, 3)], halo_recv.at[r])
        all_of(zbuf.at[r], z_recv.at[r])

        narrow = wide[:1]
        spread_lanes = [cell * SLOTS + row + 8 * h for h in range(2)]
        for x in range(4):
            for y in range(4):
                col = buf[r, x, y, 0] + wide[:4] * buf[r, x, y, 1]
                ends = [zbuf[r, e, x, y] for e in range(2)]
                ends = [e + narrow * pltpu.roll(e, 64, 1) for e in ends]
                ends = jnp.where(lane1 < 64, ends[0], ends[1])
                ends = jnp.broadcast_to(ends, (8, LANES))
                for k in range(3):
                    line = jnp.broadcast_to(col[k : k + 1], (8, LANES))
                    for h in range(2):
                        level = lane_take(line, spread_lanes[h])
                        end_lanes = jnp.where(lane < 64, 0, 64) + (k * SLOTS + 8 * h) + row
                        ghost = lane_take(ends, end_lanes)
                        expand[x * 4 + y, 0, k, h] = jnp.where(cell == DEPTH - 1, ghost, level)
                        expand[x * 4 + y, 1, k, h] = level
                        expand[x * 4 + y, 2, k, h] = jnp.where(cell == 0, ghost, level)

        def one_column(c, carry):
            base = (c // 2) * 4 + c % 2
            total = [None] * 4
            for dz in (-1, 0, 1):
                own = [jnp.broadcast_to(shifted[dz + 1, k, pl.ds(c, 1), :], (8, LANES)) for k in range(3)]
                part = [jnp.zeros((8, LANES), jnp.float32)] * 4
                for dx in (-1, 0, 1):
                    own_x = own[0] - CELL_SIDE * dx
                    for dy in (-1, 0, 1):
                        own_y = own[1] - CELL_SIDE * dy
                        other = base + (dx + 1) * 4 + dy + 1
                        for h in range(2):
                            sx = expand[other, dz + 1, 0, h] - own_x
                            sy = expand[other, dz + 1, 1, h] - own_y
                            sz = expand[other, dz + 1, 2, h] - own[2]
                            squared = sx * sx + sy * sy + sz * sz
                            inside = squared < CUTOFF * CUTOFF
                            if (dx, dy, dz) == (0, 0, 0):
                                inside = inside & (slot != row + 8 * h)
                                squared = jnp.where(inside, squared, 1.0)
                            inverse_root = lax.rsqrt(squared)
                            inverse = inverse_root * inverse_root
                            six = inverse * inverse * inverse
                            strength = (48.0 * six - 24.0) * six * inverse - FORCE_EDGE * inverse_root
                            strength = jnp.where(inside, strength, 0.0)
                            energy = (six - 1.0) * six * 4.0 + (squared * inverse_root * FORCE_EDGE + ENERGY_SHIFT)
                            energy = jnp.where(inside, energy, 0.0)
                            part[0] = part[0] - strength * sx
                            part[1] = part[1] - strength * sy
                            part[2] = part[2] - strength * sz
                            part[3] = part[3] + energy
                for k in range(4):
                    back = pltpu.roll(part[k], (-SLOTS * dz) % LANES, 1) if dz else part[k]
                    total[k] = back if total[k] is None else total[k] + back
            for k in range(4):
                acc[k, c] = total[k]
            return carry

        lax.fori_loop(0, 4, one_column, 0)

        sums = []
        for k in range(4):
            for c in range(4):
                strip[c : c + 1, :] = jnp.sum(acc[k, c], axis=0, keepdims=True)
            sums.append(jnp.where(here & (row < 4), strip[...], 0.0))
        force, energy = sums[:3], sums[3]
        vigor = jnp.zeros((8, LANES), jnp.float32)
        for k in range(3):
            velocity[k] = velocity[k] + half_step * force[k]
            vigor = vigor + velocity[k] * velocity[k]

        @pl.when(r > 0)
        def _():
            k_row = half_sum(jnp.sum(vigor, axis=0, keepdims=True), 64)
            u_row = half_sum(jnp.sum(energy, axis=0, keepdims=True), 32)
            n_row = count
            value = jnp.where(lane1 < 64, k_row, jnp.where(lane1 < 96, u_row, n_row))
            share(red_a, me_a, group_a, a_send, a_recv, r - 1, value)

        for k in range(3):
            state[VEL + k] = velocity[k]
            state[FORCE + k] = force[k]
            state[BASE + k] = position[k] + (0.5 * TIME_STEP * TIME_STEP) * force[k]
            state[TERM + k] = TIME_STEP * velocity[k]

        @pl.when(r < STEPS)
        def _():
            ship(r + 1)

        def reduced():
            value = collect(red_a, size_a, a_recv, r - 1)
            share(red_b, me_b, group_b, b_send, b_recv, r - 1, value)
            value = collect(red_b, size_b, b_recv, r - 1)
            vigor_sum = 0.5 * jnp.sum(jnp.where(lane1 < 64, value, 0.0), axis=1, keepdims=True)
            body_tally = jnp.sum(jnp.where(lane1 >= 96, value, 0.0), axis=1, keepdims=True)
            potential = 0.5 * jnp.sum(jnp.where((lane1 >= 64) & (lane1 < 96), value, 0.0), axis=1, keepdims=True)
            warmth = 2.0 * vigor_sum / (3.0 * body_tally)
            new = jnp.sqrt(1.0 + BATH_STRENGTH * (GOAL_WARMTH / warmth - 1.0))
            slot_total = float(nx * ny * nz * 4 * DEPTH * SLOTS)
            record = jnp.where(row == 0, potential, new * new * vigor_sum) / slot_total
            acc[4, 0] = jnp.where(lane == r - 1, record, acc[4, 0])
            return new

        return lax.cond(r > 0, reduced, lambda: jnp.ones((1, 1), jnp.float32))

    stretch = lax.fori_loop(0, ROUNDS, one_round, jnp.ones((1, 1), jnp.float32))

    def unflatten(line):
        lanes = row * SLOTS + slot
        return lane_take(jnp.broadcast_to(line, (8, LANES)), lanes)[:, :SLOTS]

    for c in range(4):
        for k in range(3):
            oo_ref[c // 2, c % 2, k] = unflatten(state[POS + k, c : c + 1, :])
            vo_ref[c // 2, c % 2, k] = unflatten(stretch * state[VEL + k, c : c + 1, :])
            fo_ref[c // 2, c % 2, k] = unflatten(state[FORCE + k, c : c + 1, :])
    hist_ref[...] = acc[4, 0][:2, :STEPS]

    def drain(r, carry):
        all_of(buf.at[r, pl.ds(0, 3)], halo_send.at[r])
        all_of(zbuf.at[r], z_send.at[r])
        return carry

    lax.fori_loop(0, ROUNDS, drain, 0)

    def drain_sums(k, carry):
        all_of(red_a.at[k, pl.ds(0, size_a - 1)], a_send.at[k])
        all_of(red_b.at[k, pl.ds(0, size_b - 1)], b_send.at[k])
        return carry

    lax.fori_loop(0, STEPS, drain_sums, 0)


def per_device(sizes, offsets, velocities, occupied):
    nx, ny, nz = sizes
    size_a, size_b = nz * 2, nx * (ny // 2)
    order = (0, 1, 4, 2, 3)
    block = jax.ShapeDtypeStruct((2, 2, 3, DEPTH, SLOTS), jnp.float32)
    whole = pl.BlockSpec(memory_space=pltpu.VMEM)
    dma = pltpu.SemaphoreType.DMA
    vmem = functools.partial(lambda *shape: pltpu.VMEM(shape, jnp.float32))
    position, velocity, force, history = pl.pallas_call(
        functools.partial(kernel, sizes),
        out_shape=(block, block, block, jax.ShapeDtypeStruct((2, STEPS), jnp.float32)),
        in_specs=[whole] * 3,
        out_specs=(whole,) * 4,
        scratch_shapes=[
            vmem(ROUNDS, 4, 4, 2, 4, LANES),
            vmem(ROUNDS, 2, 2, 2, 1, LANES),
            vmem(ROUNDS, 2, 4, 4, 1, LANES),
            vmem(STEPS, size_a, 1, LANES),
            vmem(STEPS, size_b, 1, LANES),
            vmem(16, 3, 3, 2, 8, LANES),
            vmem(5, 4, 8, LANES),
            vmem(16, 8, LANES),
            vmem(3, 3, 8, LANES),
            vmem(8, LANES),
            dma((ROUNDS,)), dma((ROUNDS,)), dma((ROUNDS,)), dma((ROUNDS,)),
            dma((STEPS,)), dma((STEPS,)), dma((STEPS,)), dma((STEPS,)),
        ],
        compiler_params=pltpu.CompilerParams(collective_id=0, has_side_effects=True),
        name="window",
    )(offsets.transpose(order), velocities.transpose(order), occupied)
    back = (0, 1, 3, 4, 2)
    return (position.transpose(back), velocity.transpose(back), force.transpose(back), history.T)


def solution(mesh):
    sizes = tuple(mesh.shape[a] for a in ("gx", "gy", "gz"))
    cells = P("gx", "gy", "gz", None, None)
    return jax.shard_map(
        functools.partial(per_device, sizes),
        mesh=mesh,
        in_specs=(cells, cells, P("gx", "gy", "gz", None)),
        out_specs=(cells, cells, cells, P()),
        check_vma=False,
    )
```

```python
import functools
import itertools

import jax
import jax.numpy as jnp
from jax import lax
from jax.experimental import pallas as pl
from jax.experimental.pallas import tpu as pltpu
from jax.sharding import PartitionSpec as P

STEPS = 4
ROUNDS = STEPS + 1
CUTOFF = 2.5
CELL_SIDE = 2.6
TIME_STEP = 0.005
BATH_STRENGTH = 0.25
GOAL_WARMTH = 0.8
FORCE_EDGE = 24.0 * (2.0 * CUTOFF ** (-13) - CUTOFF ** (-7))
ENERGY_EDGE = 4.0 * (CUTOFF ** (-12) - CUTOFF ** (-6))
ENERGY_SHIFT = -ENERGY_EDGE - CUTOFF * FORCE_EDGE
FAR = 1.0e6
MESH = pl.DeviceIdType.MESH
LANES = 128
SLOTS = 16
DEPTH = 8

SIDES = {0: (pl.ds(0, 2), pl.ds(1, 2)), 1: (pl.ds(1, 1), pl.ds(0, 1)), -1: (pl.ds(0, 1), pl.ds(3, 1))}
NEIGHBOURS = sorted(
    (d for d in itertools.product((-1, 0, 1), repeat=3) if d != (0, 0, 0)),
    key=lambda d: -(2 * abs(d[0]) + 2 * abs(d[1]) + abs(d[2])),
)


def lane_take(x, lanes):
    return jnp.take_along_axis(x, lanes, axis=1, mode="promise_in_bounds")


def kernel(
    sizes, o_ref, v_ref, w_ref, out_ref,
    buf, zsrc, zbuf, red_a, red_b, expand, acc, state, shifted, strip,
    halo_recv, halo_send, z_recv, z_send, a_recv, a_send, b_recv, b_send,
):
    nx, ny, nz = sizes
    gx, gy, gz = (lax.axis_index(a) for a in ("gx", "gy", "gz"))
    high, core = gy // 2, gy % 2
    n_high = ny // 2

    def at(dx, dy, dz):
        return (lax.rem(gx + dx + nx, nx), lax.rem(gy + dy + ny, ny), lax.rem(gz + dz + nz, nz))

    group_a = [
        (gx, high * 2 + lax.rem(core + dc, 2), lax.rem(gz + dz, nz))
        for dz in range(nz) for dc in range(2) if (dz, dc) != (0, 0)
    ]
    me_a = gz * 2 + core
    group_b = [
        (lax.rem(gx + dx, nx), lax.rem(high + dh, n_high) * 2 + core, gz)
        for dx in range(nx) for dh in range(n_high) if (dx, dh) != (0, 0)
    ]
    me_b = gx * n_high + high
    size_a, size_b = nz * 2, nx * n_high

    barrier = pltpu.get_barrier_semaphore()
    peers = [at(*d) for d in NEIGHBOURS] + group_a + group_b
    for peer in peers:
        pl.semaphore_signal(barrier, inc=1, device_id=peer, device_id_type=MESH)

    lane = lax.broadcasted_iota(jnp.int32, (8, LANES), 1)
    row = lax.broadcasted_iota(jnp.int32, (8, LANES), 0)
    slot, cell = lane % SLOTS, lane // SLOTS
    lane1 = lane[:1]

    def flatten(block):
        strip[:, :SLOTS] = block
        spread = lane_take(strip[...], slot)
        return jnp.sum(jnp.where(cell == row, spread, 0.0), axis=0, keepdims=True)

    for k in range(16):
        state[k] = jnp.zeros((8, LANES), jnp.float32)
    POS, VEL, FORCE, BASE, TERM, WEIGHT = 0, 3, 6, 9, 12, 15
    for c in range(4):
        cx, cy = c // 2, c % 2
        state[WEIGHT, c : c + 1, :] = flatten(w_ref[cx, cy].astype(jnp.float32))
        for k in range(3):
            state[BASE + k, c : c + 1, :] = flatten(o_ref[cx, cy, k])
            state[VEL + k, c : c + 1, :] = flatten(v_ref[cx, cy, k])
    for k in range(3):
        state[VEL + k] = state[VEL + k] * state[WEIGHT]
    acc[...] = jnp.zeros_like(acc)
    for r in range(ROUNDS):
        for cx in range(2):
            for cy in range(2):
                buf[r, 1 + cx, 1 + cy] = jnp.zeros((2, 4, LANES), jnp.float32)

    def ship(r):
        here = state[WEIGHT] > 0.5
        base = [jnp.where(here, state[BASE + k], FAR) for k in range(3)]
        term = [state[TERM + k] for k in range(3)]
        for c in range(4):
            for k in range(3):
                buf[r, 1 + c // 2, 1 + c % 2, 0, k : k + 1, :] = base[k][c : c + 1]
                buf[r, 1 + c // 2, 1 + c % 2, 1, k : k + 1, :] = term[k][c : c + 1]
        for end in range(2):
            pick = slot + end * (LANES - SLOTS)
            packed = jnp.zeros((8, LANES), jnp.float32)
            for k in range(3):
                packed = jnp.where(cell == k + 4 * end, lane_take(base[k], pick), packed)
                packed = jnp.where(cell == k + 4 - 4 * end, lane_take(term[k], pick), packed)
            for c in range(4):
                zsrc[r, end, c // 2, c % 2] = packed[c : c + 1]
        for dx, dy, dz in NEIGHBOURS:
            (from_x, to_x), (from_y, to_y) = SIDES[dx], SIDES[dy]
            if dz == 0:
                own_x, own_y = pl.ds(from_x.start + 1, from_x.size), pl.ds(from_y.start + 1, from_y.size)
                pltpu.make_async_remote_copy(
                    src_ref=buf.at[r, own_x, own_y], dst_ref=buf.at[r, to_x, to_y],
                    send_sem=halo_send.at[r], recv_sem=halo_recv.at[r],
                    device_id=at(dx, dy, dz), device_id_type=MESH,
                ).start()
            else:
                end = 0 if dz < 0 else 1
                pltpu.make_async_remote_copy(
                    src_ref=zsrc.at[r, end, from_x, from_y], dst_ref=zbuf.at[r, end, to_x, to_y],
                    send_sem=z_send.at[r], recv_sem=z_recv.at[r],
                    device_id=at(dx, dy, dz), device_id_type=MESH,
                ).start()

    def all_of(ref, sem):
        pltpu.make_async_copy(ref, ref, sem).wait()

    def share(stage, me, group, send_sem, recv_sem, k, value):
        stage[k, me] = value
        for peer in group:
            pltpu.make_async_remote_copy(
                src_ref=stage.at[k, me], dst_ref=stage.at[k, me],
                send_sem=send_sem.at[k], recv_sem=recv_sem.at[k],
                device_id=peer, device_id_type=MESH,
            ).start()

    def collect(stage, size, recv_sem, k):
        all_of(stage.at[k, pl.ds(0, size - 1)], recv_sem.at[k])
        return jnp.sum(stage[k], axis=0)

    def half_sum(value, width):
        while width < LANES:
            value = value + pltpu.roll(value, width, 1)
            width *= 2
        return value

    count = jnp.sum(state[WEIGHT], axis=0, keepdims=True)
    count = count + pltpu.roll(count, 64, 1)
    count = count + pltpu.roll(count, 32, 1)

    pl.semaphore_wait(barrier, len(peers))
    ship(0)

    def one_round(r, stretch):
        wide = jnp.broadcast_to(stretch, (8, LANES))
        half_step = jnp.where(r == 0, 0.0, 0.5 * TIME_STEP)
        here = state[WEIGHT] > 0.5
        position, velocity = [], []
        for k in range(3):
            position.append(state[BASE + k] + wide * state[TERM + k])
            velocity.append(wide * state[VEL + k] + (0.5 * TIME_STEP) * state[FORCE + k])
            state[POS + k] = position[k]
            for dz in (-1, 0, 1):
                moved = pltpu.roll(position[k], (SLOTS * dz) % LANES, 1) if dz else position[k]
                shifted[dz + 1, k] = moved - CELL_SIDE * dz if k == 2 else moved

        all_of(buf.at[r, pl.ds(0, 3)], halo_recv.at[r])
        all_of(zbuf.at[r], z_recv.at[r])

        narrow = wide[:1]
        spread_lanes = [cell * SLOTS + row + 8 * h for h in range(2)]
        for x in range(4):
            for y in range(4):
                col = buf[r, x, y, 0] + wide[:4] * buf[r, x, y, 1]
                ends = [zbuf[r, e, x, y] for e in range(2)]
                ends = [e + narrow * pltpu.roll(e, 64, 1) for e in ends]
                ends = jnp.where(lane1 < 64, ends[0], ends[1])
                ends = jnp.broadcast_to(ends, (8, LANES))
                for k in range(3):
                    line = jnp.broadcast_to(col[k : k + 1], (8, LANES))
                    for h in range(2):
                        level = lane_take(line, spread_lanes[h])
                        end_lanes = jnp.where(lane < 64, 0, 64) + (k * SLOTS + 8 * h) + row
                        ghost = lane_take(ends, end_lanes)
                        expand[x * 4 + y, 0, k, h] = jnp.where(cell == DEPTH - 1, ghost, level)
                        expand[x * 4 + y, 1, k, h] = level
                        expand[x * 4 + y, 2, k, h] = jnp.where(cell == 0, ghost, level)

        def one_column(c, carry):
            base = (c // 2) * 4 + c % 2
            total = [None] * 4
            for dz in (-1, 0, 1):
                own = [jnp.broadcast_to(shifted[dz + 1, k, pl.ds(c, 1), :], (8, LANES)) for k in range(3)]
                part = [jnp.zeros((8, LANES), jnp.float32)] * 4
                for dx in (-1, 0, 1):
                    own_x = own[0] - CELL_SIDE * dx
                    for dy in (-1, 0, 1):
                        own_y = own[1] - CELL_SIDE * dy
                        other = base + (dx + 1) * 4 + dy + 1
                        for h in range(2):
                            sx = expand[other, dz + 1, 0, h] - own_x
                            sy = expand[other, dz + 1, 1, h] - own_y
                            sz = expand[other, dz + 1, 2, h] - own[2]
                            squared = sx * sx + sy * sy + sz * sz
                            inside = squared < CUTOFF * CUTOFF
                            if (dx, dy, dz) == (0, 0, 0):
                                inside = inside & (slot != row + 8 * h)
                                squared = jnp.where(inside, squared, 1.0)
                            inverse_root = lax.rsqrt(squared)
                            inverse = inverse_root * inverse_root
                            six = inverse * inverse * inverse
                            strength = (48.0 * six - 24.0) * six * inverse - FORCE_EDGE * inverse_root
                            strength = jnp.where(inside, strength, 0.0)
                            energy = (six - 1.0) * six * 4.0 + (squared * inverse_root * FORCE_EDGE + ENERGY_SHIFT)
                            energy = jnp.where(inside, energy, 0.0)
                            part[0] = part[0] - strength * sx
                            part[1] = part[1] - strength * sy
                            part[2] = part[2] - strength * sz
                            part[3] = part[3] + energy
                for k in range(4):
                    back = pltpu.roll(part[k], (-SLOTS * dz) % LANES, 1) if dz else part[k]
                    total[k] = back if total[k] is None else total[k] + back
            for k in range(4):
                acc[k, c] = total[k]
            return carry

        lax.fori_loop(0, 4, one_column, 0)

        sums = []
        for k in range(4):
            for c in range(4):
                strip[c : c + 1, :] = jnp.sum(acc[k, c], axis=0, keepdims=True)
            sums.append(jnp.where(here & (row < 4), strip[...], 0.0))
        force, energy = sums[:3], sums[3]
        vigor = jnp.zeros((8, LANES), jnp.float32)
        for k in range(3):
            velocity[k] = velocity[k] + half_step * force[k]
            vigor = vigor + velocity[k] * velocity[k]

        @pl.when(r > 0)
        def _():
            k_row = half_sum(jnp.sum(vigor, axis=0, keepdims=True), 64)
            u_row = half_sum(jnp.sum(energy, axis=0, keepdims=True), 32)
            n_row = count
            value = jnp.where(lane1 < 64, k_row, jnp.where(lane1 < 96, u_row, n_row))
            share(red_a, me_a, group_a, a_send, a_recv, r - 1, value)

        for k in range(3):
            state[VEL + k] = velocity[k]
            state[FORCE + k] = force[k]
            state[BASE + k] = position[k] + (0.5 * TIME_STEP * TIME_STEP) * force[k]
            state[TERM + k] = TIME_STEP * velocity[k]

        @pl.when(r < STEPS)
        def _():
            ship(r + 1)

        def reduced():
            value = collect(red_a, size_a, a_recv, r - 1)
            share(red_b, me_b, group_b, b_send, b_recv, r - 1, value)
            value = collect(red_b, size_b, b_recv, r - 1)
            vigor_sum = 0.5 * jnp.sum(jnp.where(lane1 < 64, value, 0.0), axis=1, keepdims=True)
            body_tally = jnp.sum(jnp.where(lane1 >= 96, value, 0.0), axis=1, keepdims=True)
            potential = 0.5 * jnp.sum(jnp.where((lane1 >= 64) & (lane1 < 96), value, 0.0), axis=1, keepdims=True)
            warmth = 2.0 * vigor_sum / (3.0 * body_tally)
            new = jnp.sqrt(1.0 + BATH_STRENGTH * (GOAL_WARMTH / warmth - 1.0))
            slot_total = float(nx * ny * nz * 4 * DEPTH * SLOTS)
            record = jnp.where(row == 0, potential, new * new * vigor_sum) / slot_total
            acc[4, 0] = jnp.where(lane == r - 1, record, acc[4, 0])
            return new

        return lax.cond(r > 0, reduced, lambda: jnp.ones((1, 1), jnp.float32))

    stretch = lax.fori_loop(0, ROUNDS, one_round, jnp.ones((1, 1), jnp.float32))

    for k in range(3):
        out_ref[k] = state[POS + k]
        out_ref[3 + k] = stretch * state[VEL + k]
        out_ref[6 + k] = state[FORCE + k]
    out_ref[9] = acc[4, 0]

    def drain(r, carry):
        all_of(buf.at[r, pl.ds(0, 3)], halo_send.at[r])
        all_of(zbuf.at[r], z_send.at[r])
        return carry

    lax.fori_loop(0, ROUNDS, drain, 0)

    def drain_sums(k, carry):
        all_of(red_a.at[k, pl.ds(0, size_a - 1)], a_send.at[k])
        all_of(red_b.at[k, pl.ds(0, size_b - 1)], b_send.at[k])
        return carry

    lax.fori_loop(0, STEPS, drain_sums, 0)


def unfold(in_ref, oo_ref, vo_ref, fo_ref, hist_ref):
    lane = lax.broadcasted_iota(jnp.int32, (8, LANES), 1)
    row = lax.broadcasted_iota(jnp.int32, (8, LANES), 0)
    lanes = row * SLOTS + lane % SLOTS
    for n, ref in enumerate((oo_ref, vo_ref, fo_ref)):
        for k in range(3):
            for c in range(4):
                line = jnp.broadcast_to(in_ref[3 * n + k, c : c + 1, :], (8, LANES))
                ref[c // 2, c % 2, k] = lane_take(line, lanes)[:, :SLOTS]
    hist_ref[...] = in_ref[9, :2, :STEPS]


def per_device(sizes, offsets, velocities, occupied):
    nx, ny, nz = sizes
    size_a, size_b = nz * 2, nx * (ny // 2)
    order = (0, 1, 4, 2, 3)
    block = jax.ShapeDtypeStruct((2, 2, 3, DEPTH, SLOTS), jnp.float32)
    whole = pl.BlockSpec(memory_space=pltpu.VMEM)
    dma = pltpu.SemaphoreType.DMA
    vmem = functools.partial(lambda *shape: pltpu.VMEM(shape, jnp.float32))
    lines = pl.pallas_call(
        functools.partial(kernel, sizes),
        out_shape=pltpu.VMEM((10, 8, LANES), jnp.float32),
        in_specs=[whole] * 3,
        out_specs=whole,
        scratch_shapes=[
            vmem(ROUNDS, 4, 4, 2, 4, LANES),
            vmem(ROUNDS, 2, 2, 2, 1, LANES),
            vmem(ROUNDS, 2, 4, 4, 1, LANES),
            vmem(STEPS, size_a, 1, LANES),
            vmem(STEPS, size_b, 1, LANES),
            vmem(16, 3, 3, 2, 8, LANES),
            vmem(5, 4, 8, LANES),
            vmem(16, 8, LANES),
            vmem(3, 3, 8, LANES),
            vmem(8, LANES),
            dma((ROUNDS,)), dma((ROUNDS,)), dma((ROUNDS,)), dma((ROUNDS,)),
            dma((STEPS,)), dma((STEPS,)), dma((STEPS,)), dma((STEPS,)),
        ],
        compiler_params=pltpu.CompilerParams(collective_id=0, has_side_effects=True),
        name="window",
    )(offsets.transpose(order), velocities.transpose(order), occupied)
    position, velocity, force, history = pl.pallas_call(
        unfold,
        out_shape=(block, block, block, jax.ShapeDtypeStruct((2, STEPS), jnp.float32)),
        in_specs=[whole],
        out_specs=(whole,) * 4,
        name="unfold",
    )(pltpu.with_memory_space_constraint(lines, pltpu.VMEM))
    back = (0, 1, 3, 4, 2)
    return (position.transpose(back), velocity.transpose(back), force.transpose(back), history.T)


def solution(mesh):
    sizes = tuple(mesh.shape[a] for a in ("gx", "gy", "gz"))
    cells = P("gx", "gy", "gz", None, None)
    return jax.shard_map(
        functools.partial(per_device, sizes),
        mesh=mesh,
        in_specs=(cells, cells, P("gx", "gy", "gz", None)),
        out_specs=(cells, cells, cells, P()),
        check_vma=False,
    )
```

```python
import functools
import itertools

import jax
import jax.numpy as jnp
from jax import lax
from jax.experimental import pallas as pl
from jax.experimental.pallas import tpu as pltpu
from jax.sharding import PartitionSpec as P

STEPS = 4
ROUNDS = STEPS + 1
CUTOFF = 2.5
CELL_SIDE = 2.6
TIME_STEP = 0.005
BATH_STRENGTH = 0.25
GOAL_WARMTH = 0.8
FORCE_EDGE = 24.0 * (2.0 * CUTOFF ** (-13) - CUTOFF ** (-7))
ENERGY_EDGE = 4.0 * (CUTOFF ** (-12) - CUTOFF ** (-6))
ENERGY_SHIFT = -ENERGY_EDGE - CUTOFF * FORCE_EDGE
UNIT = 2.0 ** (1.0 / 6.0)
SIDE = CELL_SIDE / UNIT
EDGE = FORCE_EDGE * UNIT / 12.0
FAR = 1.0e6
MESH = pl.DeviceIdType.MESH
LANES = 128
SLOTS = 16
DEPTH = 8

SIDES = {0: (pl.ds(0, 2), pl.ds(1, 2)), 1: (pl.ds(1, 1), pl.ds(0, 1)), -1: (pl.ds(0, 1), pl.ds(3, 1))}
NEIGHBOURS = sorted(
    (d for d in itertools.product((-1, 0, 1), repeat=3) if d != (0, 0, 0)),
    key=lambda d: -(2 * abs(d[0]) + 2 * abs(d[1]) + abs(d[2])),
)


def lane_take(x, lanes):
    return jnp.take_along_axis(x, lanes, axis=1, mode="promise_in_bounds")


def kernel(
    sizes, o_hbm, v_hbm, w_hbm, out_ref, o_ref, v_ref, w_ref, in_sem,
    buf, zsrc, zbuf, red_a, red_b, lines, expand, acc, state, shifted, strip,
    halo_recv, halo_send, z_recv, z_send, a_recv, a_send, b_recv, b_send,
):
    nx, ny, nz = sizes
    gx, gy, gz = (lax.axis_index(a) for a in ("gx", "gy", "gz"))
    high, core = gy // 2, gy % 2
    n_high = ny // 2

    def at(dx, dy, dz):
        return (lax.rem(gx + dx + nx, nx), lax.rem(gy + dy + ny, ny), lax.rem(gz + dz + nz, nz))

    group_a = [
        (gx, high * 2 + lax.rem(core + dc, 2), lax.rem(gz + dz, nz))
        for dz in range(nz) for dc in range(2) if (dz, dc) != (0, 0)
    ]
    me_a = gz * 2 + core
    group_b = [
        (lax.rem(gx + dx, nx), lax.rem(high + dh, n_high) * 2 + core, gz)
        for dx in range(nx) for dh in range(n_high) if (dx, dh) != (0, 0)
    ]
    me_b = gx * n_high + high
    size_a, size_b = nz * 2, nx * n_high

    barrier = pltpu.get_barrier_semaphore()
    peers = [at(*d) for d in NEIGHBOURS] + group_a + group_b
    for peer in peers:
        pl.semaphore_signal(barrier, inc=1, device_id=peer, device_id_type=MESH)

    fetches = [
        pltpu.make_async_copy(src, dst, in_sem.at[n])
        for n, (src, dst) in enumerate(((o_hbm, o_ref), (v_hbm, v_ref), (w_hbm, w_ref)))
    ]
    for fetch in fetches:
        fetch.start()

    lane = lax.broadcasted_iota(jnp.int32, (8, LANES), 1)
    row = lax.broadcasted_iota(jnp.int32, (8, LANES), 0)
    slot, cell = lane % SLOTS, lane // SLOTS
    lane1 = lane[:1]

    def flatten(n, block):
        expand[n // 18, n // 6 % 3, n // 2 % 3, n % 2, :, :SLOTS] = block
        spread = lane_take(expand[n // 18, n // 6 % 3, n // 2 % 3, n % 2], slot)
        return jnp.sum(jnp.where(cell == row, spread, 0.0), axis=0, keepdims=True)

    for k in range(16):
        state[k] = jnp.zeros((8, LANES), jnp.float32)
    POS, VEL, FORCE, BASE, TERM, WEIGHT = 0, 3, 6, 9, 12, 15
    for fetch in fetches:
        fetch.wait()
    for c in range(4):
        cx, cy = c // 2, c % 2
        state[WEIGHT, c : c + 1, :] = flatten(7 * c, w_ref[cx, cy].astype(jnp.float32))
        for k in range(3):
            state[BASE + k, c : c + 1, :] = flatten(7 * c + 1 + k, o_ref[cx, cy, k])
            state[VEL + k, c : c + 1, :] = flatten(7 * c + 4 + k, v_ref[cx, cy, k])
    for k in range(3):
        state[VEL + k] = state[VEL + k] * state[WEIGHT]
    acc[...] = jnp.zeros_like(acc)
    for r in range(ROUNDS):
        for cx in range(2):
            for cy in range(2):
                buf[r, 1 + cx, 1 + cy] = jnp.zeros((2, 4, LANES), jnp.float32)

    def ship(r):
        here = state[WEIGHT] > 0.5
        base = [jnp.where(here, state[BASE + k], FAR) for k in range(3)]
        term = [state[TERM + k] for k in range(3)]
        for c in range(4):
            for k in range(3):
                buf[r, 1 + c // 2, 1 + c % 2, 0, k : k + 1, :] = base[k][c : c + 1]
                buf[r, 1 + c // 2, 1 + c % 2, 1, k : k + 1, :] = term[k][c : c + 1]
        for end in range(2):
            pick = slot + end * (LANES - SLOTS)
            packed = jnp.zeros((8, LANES), jnp.float32)
            for k in range(3):
                place = (2 * k + (DEPTH - 1) * end) % DEPTH
                packed = jnp.where(cell == place, lane_take(base[k], pick), packed)
                packed = jnp.where(cell == (place + 1) % DEPTH, lane_take(term[k], pick), packed)
            for c in range(4):
                zsrc[r, end, c // 2, c % 2] = packed[c : c + 1]
        for dx, dy, dz in NEIGHBOURS:
            (from_x, to_x), (from_y, to_y) = SIDES[dx], SIDES[dy]
            if dz == 0:
                own_x, own_y = pl.ds(from_x.start + 1, from_x.size), pl.ds(from_y.start + 1, from_y.size)
                pltpu.make_async_remote_copy(
                    src_ref=buf.at[r, own_x, own_y], dst_ref=buf.at[r, to_x, to_y],
                    send_sem=halo_send.at[r], recv_sem=halo_recv.at[r],
                    device_id=at(dx, dy, dz), device_id_type=MESH,
                ).start()
            else:
                end = 0 if dz < 0 else 1
                pltpu.make_async_remote_copy(
                    src_ref=zsrc.at[r, end, from_x, from_y], dst_ref=zbuf.at[r, end, to_x, to_y],
                    send_sem=z_send.at[r], recv_sem=z_recv.at[r],
                    device_id=at(dx, dy, dz), device_id_type=MESH,
                ).start()

    def all_of(ref, sem):
        pltpu.make_async_copy(ref, ref, sem).wait()

    def share(stage, me, group, send_sem, recv_sem, k, value):
        stage[k, me] = value
        for peer in group:
            pltpu.make_async_remote_copy(
                src_ref=stage.at[k, me], dst_ref=stage.at[k, me],
                send_sem=send_sem.at[k], recv_sem=recv_sem.at[k],
                device_id=peer, device_id_type=MESH,
            ).start()

    def collect(stage, size, recv_sem, k):
        all_of(stage.at[k, pl.ds(0, size - 1)], recv_sem.at[k])
        return jnp.sum(stage[k], axis=0)

    def half_sum(value, width):
        while width < LANES:
            value = value + pltpu.roll(value, width, 1)
            width *= 2
        return value

    count = jnp.sum(state[WEIGHT], axis=0, keepdims=True)
    count = count + pltpu.roll(count, 64, 1)
    count = count + pltpu.roll(count, 32, 1)

    pl.semaphore_wait(barrier, len(peers))
    ship(0)

    def one_round(r, stretch):
        wide = jnp.broadcast_to(stretch, (8, LANES))
        half_step = jnp.where(r == 0, 0.0, 0.5 * TIME_STEP)
        here = state[WEIGHT] > 0.5
        position, velocity = [], []
        for k in range(3):
            position.append(state[BASE + k] + wide * state[TERM + k])
            velocity.append(wide * state[VEL + k] + (0.5 * TIME_STEP) * state[FORCE + k])
            state[POS + k] = position[k]
            for dz in (-1, 0, 1):
                moved = position[k] * (1.0 / UNIT)
                moved = pltpu.roll(moved, (SLOTS * dz) % LANES, 1) if dz else moved
                shifted[dz + 1, k] = moved - SIDE * dz if k == 2 else moved

        all_of(buf.at[r, pl.ds(0, 3)], halo_recv.at[r])
        all_of(zbuf.at[r], z_recv.at[r])

        narrow = wide[:1]
        for x in range(4):
            for y in range(4):
                lines[x * 4 + y, 0] = (buf[r, x, y, 0] + wide[:4] * buf[r, x, y, 1]) * (1.0 / UNIT)
                ends = [zbuf[r, e, x, y] for e in range(2)]
                ends = [e + narrow * pltpu.roll(e, LANES - SLOTS, 1) for e in ends]
                ends = jnp.where(cell[:1] % 2 == 0, ends[0], ends[1]) * (1.0 / UNIT)
                for k in range(3):
                    turned = pltpu.roll(ends, LANES - 2 * SLOTS * k, 1) if k else ends
                    lines[x * 4 + y, 1, k : k + 1, :] = turned
        for h in range(2):
            spread_lanes = cell * SLOTS + row + 8 * h
            for n in range(16):
                for k in range(3):
                    level, ghost = (
                        lane_take(jnp.broadcast_to(lines[n, e, k : k + 1, :], (8, LANES)), spread_lanes)
                        for e in range(2)
                    )
                    expand[n, 0, k, h] = jnp.where(cell == DEPTH - 1, ghost, level)
                    expand[n, 1, k, h] = level
                    expand[n, 2, k, h] = jnp.where(cell == 0, ghost, level)

        def one_column(c, carry):
            base = (c // 2) * 4 + c % 2
            total = [None] * 4
            for dz in (-1, 0, 1):
                own = [jnp.broadcast_to(shifted[dz + 1, k, pl.ds(c, 1), :], (8, LANES)) for k in range(3)]
                part = [jnp.zeros((8, LANES), jnp.float32)] * 4
                for dx in (-1, 0, 1):
                    own_x = own[0] - SIDE * dx
                    for dy in (-1, 0, 1):
                        own_y = own[1] - SIDE * dy
                        other = base + (dx + 1) * 4 + dy + 1
                        for h in range(2):
                            sx = expand[other, dz + 1, 0, h] - own_x
                            sy = expand[other, dz + 1, 1, h] - own_y
                            sz = expand[other, dz + 1, 2, h] - own[2]
                            squared = sx * sx + sy * sy + sz * sz
                            inside = squared < (CUTOFF / UNIT) ** 2
                            if (dx, dy, dz) == (0, 0, 0):
                                inside = inside & (slot != row + 8 * h)
                                squared = jnp.where(inside, squared, 1.0)
                            inverse_root = lax.rsqrt(squared)
                            inverse = inverse_root * inverse_root
                            six = inverse * inverse * inverse
                            wall = six * (six - 1.0)
                            strength = jnp.where(inside, wall * inverse - EDGE * inverse_root, 0.0)
                            energy = (wall - six) + (squared * inverse_root * (12.0 * EDGE) + ENERGY_SHIFT)
                            part[0] = part[0] + strength * sx
                            part[1] = part[1] + strength * sy
                            part[2] = part[2] + strength * sz
                            part[3] = part[3] + jnp.where(inside, energy, 0.0)
                for k in range(4):
                    back = pltpu.roll(part[k], (-SLOTS * dz) % LANES, 1) if dz else part[k]
                    total[k] = back if total[k] is None else total[k] + back
            for k in range(4):
                acc[k, c] = total[k]
            return carry

        lax.fori_loop(0, 4, one_column, 0)

        sums = []
        for k in range(4):
            for c in range(4):
                strip[c : c + 1, :] = jnp.sum(acc[k, c], axis=0, keepdims=True)
            sums.append(jnp.where(here & (row < 4), strip[...], 0.0))
        force, energy = [total * (-12.0 / UNIT) for total in sums[:3]], sums[3]
        vigor = jnp.zeros((8, LANES), jnp.float32)
        for k in range(3):
            velocity[k] = velocity[k] + half_step * force[k]
            vigor = vigor + velocity[k] * velocity[k]

        @pl.when(r > 0)
        def _():
            k_row = half_sum(jnp.sum(vigor, axis=0, keepdims=True), 64)
            u_row = half_sum(jnp.sum(energy, axis=0, keepdims=True), 32)
            n_row = count
            value = jnp.where(lane1 < 64, k_row, jnp.where(lane1 < 96, u_row, n_row))
            share(red_a, me_a, group_a, a_send, a_recv, r - 1, value)

        for k in range(3):
            state[VEL + k] = velocity[k]
            state[FORCE + k] = force[k]
            state[BASE + k] = position[k] + (0.5 * TIME_STEP * TIME_STEP) * force[k]
            state[TERM + k] = TIME_STEP * velocity[k]

        @pl.when(r < STEPS)
        def _():
            ship(r + 1)

        def reduced():
            value = collect(red_a, size_a, a_recv, r - 1)
            share(red_b, me_b, group_b, b_send, b_recv, r - 1, value)
            value = collect(red_b, size_b, b_recv, r - 1)
            vigor_sum = 0.5 * jnp.sum(jnp.where(lane1 < 64, value, 0.0), axis=1, keepdims=True)
            body_tally = jnp.sum(jnp.where(lane1 >= 96, value, 0.0), axis=1, keepdims=True)
            potential = 0.5 * jnp.sum(jnp.where((lane1 >= 64) & (lane1 < 96), value, 0.0), axis=1, keepdims=True)
            warmth = 2.0 * vigor_sum / (3.0 * body_tally)
            new = jnp.sqrt(1.0 + BATH_STRENGTH * (GOAL_WARMTH / warmth - 1.0))
            slot_total = float(nx * ny * nz * 4 * DEPTH * SLOTS)
            record = jnp.where(row == 0, potential, new * new * vigor_sum) / slot_total
            acc[4, 0] = jnp.where(lane == r - 1, record, acc[4, 0])
            return new

        return lax.cond(r > 0, reduced, lambda: jnp.ones((1, 1), jnp.float32))

    stretch = lax.fori_loop(0, ROUNDS, one_round, jnp.ones((1, 1), jnp.float32))

    for k in range(3):
        out_ref[k] = state[POS + k]
        out_ref[3 + k] = stretch * state[VEL + k]
        out_ref[6 + k] = state[FORCE + k]
    out_ref[9] = acc[4, 0]

    def drain(r, carry):
        all_of(buf.at[r, pl.ds(0, 3)], halo_send.at[r])
        all_of(zbuf.at[r], z_send.at[r])
        return carry

    lax.fori_loop(0, ROUNDS, drain, 0)

    def drain_sums(k, carry):
        all_of(red_a.at[k, pl.ds(0, size_a - 1)], a_send.at[k])
        all_of(red_b.at[k, pl.ds(0, size_b - 1)], b_send.at[k])
        return carry

    lax.fori_loop(0, STEPS, drain_sums, 0)


def unfold(in_ref, oo_ref, vo_ref, fo_ref, hist_ref):
    lane = lax.broadcasted_iota(jnp.int32, (8, LANES), 1)
    row = lax.broadcasted_iota(jnp.int32, (8, LANES), 0)
    lanes = row * SLOTS + lane % SLOTS
    for n, ref in enumerate((oo_ref, vo_ref, fo_ref)):
        for k in range(3):
            for c in range(4):
                line = jnp.broadcast_to(in_ref[3 * n + k, c : c + 1, :], (8, LANES))
                ref[c // 2, c % 2, k] = lane_take(line, lanes)[:, :SLOTS]
    hist_ref[...] = in_ref[9, :2, :STEPS]


def per_device(sizes, offsets, velocities, occupied):
    nx, ny, nz = sizes
    size_a, size_b = nz * 2, nx * (ny // 2)
    order = (0, 1, 4, 2, 3)
    block = jax.ShapeDtypeStruct((2, 2, 3, DEPTH, SLOTS), jnp.float32)
    whole = pl.BlockSpec(memory_space=pltpu.VMEM)
    dma = pltpu.SemaphoreType.DMA
    vmem = functools.partial(lambda *shape: pltpu.VMEM(shape, jnp.float32))
    lines = pl.pallas_call(
        functools.partial(kernel, sizes),
        out_shape=pltpu.VMEM((10, 8, LANES), jnp.float32),
        in_specs=[pl.BlockSpec(memory_space=pl.ANY)] * 3,
        out_specs=whole,
        scratch_shapes=[
            vmem(2, 2, 3, DEPTH, SLOTS), vmem(2, 2, 3, DEPTH, SLOTS), pltpu.VMEM((2, 2, DEPTH, SLOTS), jnp.int32), dma((3,)),
            vmem(ROUNDS, 4, 4, 2, 4, LANES),
            vmem(ROUNDS, 2, 2, 2, 1, LANES),
            vmem(ROUNDS, 2, 4, 4, 1, LANES),
            vmem(STEPS, size_a, 1, LANES),
            vmem(STEPS, size_b, 1, LANES),
            vmem(16, 2, 4, LANES),
            vmem(16, 3, 3, 2, 8, LANES),
            vmem(5, 4, 8, LANES),
            vmem(16, 8, LANES),
            vmem(3, 3, 8, LANES),
            vmem(8, LANES),
            dma((ROUNDS,)), dma((ROUNDS,)), dma((ROUNDS,)), dma((ROUNDS,)),
            dma((STEPS,)), dma((STEPS,)), dma((STEPS,)), dma((STEPS,)),
        ],
        compiler_params=pltpu.CompilerParams(collective_id=0, has_side_effects=True),
        name="window",
    )(offsets.transpose(order), velocities.transpose(order), occupied)
    position, velocity, force, history = pl.pallas_call(
        unfold,
        out_shape=(block, block, block, jax.ShapeDtypeStruct((2, STEPS), jnp.float32)),
        in_specs=[whole],
        out_specs=(whole,) * 4,
        name="unfold",
    )(pltpu.with_memory_space_constraint(lines, pltpu.VMEM))
    back = (0, 1, 3, 4, 2)
    return (position.transpose(back), velocity.transpose(back), force.transpose(back), history.T)


def solution(mesh):
    sizes = tuple(mesh.shape[a] for a in ("gx", "gy", "gz"))
    cells = P("gx", "gy", "gz", None, None)
    return jax.shard_map(
        functools.partial(per_device, sizes),
        mesh=mesh,
        in_specs=(cells, cells, P("gx", "gy", "gz", None)),
        out_specs=(cells, cells, cells, P()),
        check_vma=False,
    )
```

```python
import functools
import itertools

import jax
import jax.numpy as jnp
from jax import lax
from jax.experimental import pallas as pl
from jax.experimental.pallas import tpu as pltpu
from jax.sharding import PartitionSpec as P

STEPS = 4
ROUNDS = STEPS + 1
CUTOFF = 2.5
CELL_SIDE = 2.6
TIME_STEP = 0.005
BATH_STRENGTH = 0.25
GOAL_WARMTH = 0.8
FORCE_EDGE = 24.0 * (2.0 * CUTOFF ** (-13) - CUTOFF ** (-7))
ENERGY_EDGE = 4.0 * (CUTOFF ** (-12) - CUTOFF ** (-6))
ENERGY_SHIFT = -ENERGY_EDGE - CUTOFF * FORCE_EDGE
UNIT = 2.0 ** (1.0 / 6.0)
SIDE = CELL_SIDE / UNIT
EDGE = FORCE_EDGE * UNIT / 12.0
FAR = 1.0e6
MESH = pl.DeviceIdType.MESH
LANES = 128
SLOTS = 16
DEPTH = 8

SIDES = {0: (pl.ds(0, 2), pl.ds(1, 2)), 1: (pl.ds(1, 1), pl.ds(0, 1)), -1: (pl.ds(0, 1), pl.ds(3, 1))}
NEIGHBOURS = sorted(
    (d for d in itertools.product((-1, 0, 1), repeat=3) if d != (0, 0, 0)),
    key=lambda d: -(2 * abs(d[0]) + 2 * abs(d[1]) + abs(d[2])),
)


def lane_take(x, lanes):
    return jnp.take_along_axis(x, lanes, axis=1, mode="promise_in_bounds")


def kernel(
    sizes, o_hbm, v_hbm, w_hbm, out_ref, o_ref, v_ref, w_ref, in_sem,
    buf, zsrc, zbuf, red_a, red_b, lines, expand, acc, state, shifted, strip,
    halo_recv, halo_send, z_recv, z_send, a_recv, a_send, b_recv, b_send,
):
    nx, ny, nz = sizes
    gx, gy, gz = (lax.axis_index(a) for a in ("gx", "gy", "gz"))
    high, core = gy // 2, gy % 2
    n_high = ny // 2

    def at(dx, dy, dz):
        return (lax.rem(gx + dx + nx, nx), lax.rem(gy + dy + ny, ny), lax.rem(gz + dz + nz, nz))

    group_a = [
        (gx, high * 2 + lax.rem(core + dc, 2), lax.rem(gz + dz, nz))
        for dz in range(nz) for dc in range(2) if (dz, dc) != (0, 0)
    ]
    me_a = gz * 2 + core
    group_b = [
        (lax.rem(gx + dx, nx), lax.rem(high + dh, n_high) * 2 + core, gz)
        for dx in range(nx) for dh in range(n_high) if (dx, dh) != (0, 0)
    ]
    me_b = gx * n_high + high
    size_a, size_b = nz * 2, nx * n_high

    barrier = pltpu.get_barrier_semaphore()
    peers = [at(*d) for d in NEIGHBOURS] + group_a + group_b
    for peer in peers:
        pl.semaphore_signal(barrier, inc=1, device_id=peer, device_id_type=MESH)

    fetches = [
        pltpu.make_async_copy(src, dst, in_sem.at[n])
        for n, (src, dst) in enumerate(((o_hbm, o_ref), (v_hbm, v_ref), (w_hbm, w_ref)))
    ]
    for fetch in fetches:
        fetch.start()

    lane = lax.broadcasted_iota(jnp.int32, (8, LANES), 1)
    row = lax.broadcasted_iota(jnp.int32, (8, LANES), 0)
    slot, cell = lane % SLOTS, lane // SLOTS
    lane1 = lane[:1]

    def flatten(n, block):
        expand[n // 18, n // 6 % 3, n // 2 % 3, n % 2, :, :SLOTS] = block
        spread = lane_take(expand[n // 18, n // 6 % 3, n // 2 % 3, n % 2], slot)
        return jnp.sum(jnp.where(cell == row, spread, 0.0), axis=0, keepdims=True)

    for k in range(16):
        state[k] = jnp.zeros((8, LANES), jnp.float32)
    POS, VEL, FORCE, BASE, TERM, WEIGHT = 0, 3, 6, 9, 12, 15
    for fetch in fetches:
        fetch.wait()
    for c in range(4):
        cx, cy = c // 2, c % 2
        state[WEIGHT, c : c + 1, :] = flatten(7 * c, w_ref[cx, cy].astype(jnp.float32))
        for k in range(3):
            state[BASE + k, c : c + 1, :] = flatten(7 * c + 1 + k, o_ref[cx, cy, k])
            state[VEL + k, c : c + 1, :] = flatten(7 * c + 4 + k, v_ref[cx, cy, k])
    for k in range(3):
        state[VEL + k] = state[VEL + k] * state[WEIGHT]
    acc[...] = jnp.zeros_like(acc)
    for r in range(ROUNDS):
        for cx in range(2):
            for cy in range(2):
                buf[r, 1 + cx, 1 + cy] = jnp.zeros((2, 4, LANES), jnp.float32)

    def ship(r):
        here = state[WEIGHT] > 0.5
        base = [jnp.where(here, state[BASE + k], FAR) for k in range(3)]
        term = [state[TERM + k] for k in range(3)]
        for c in range(4):
            for k in range(3):
                buf[r, 1 + c // 2, 1 + c % 2, 0, k : k + 1, :] = base[k][c : c + 1]
                buf[r, 1 + c // 2, 1 + c % 2, 1, k : k + 1, :] = term[k][c : c + 1]
        for end in range(2):
            pick = slot + end * (LANES - SLOTS)
            packed = jnp.zeros((8, LANES), jnp.float32)
            for k in range(3):
                place = (2 * k + (DEPTH - 1) * end) % DEPTH
                packed = jnp.where(cell == place, lane_take(base[k], pick), packed)
                packed = jnp.where(cell == (place + 1) % DEPTH, lane_take(term[k], pick), packed)
            for c in range(4):
                zsrc[r, end, c // 2, c % 2] = packed[c : c + 1]
        for dx, dy, dz in NEIGHBOURS:
            (from_x, to_x), (from_y, to_y) = SIDES[dx], SIDES[dy]
            if dz == 0:
                own_x, own_y = pl.ds(from_x.start + 1, from_x.size), pl.ds(from_y.start + 1, from_y.size)
                pltpu.make_async_remote_copy(
                    src_ref=buf.at[r, own_x, own_y], dst_ref=buf.at[r, to_x, to_y],
                    send_sem=halo_send.at[r], recv_sem=halo_recv.at[r],
                    device_id=at(dx, dy, dz), device_id_type=MESH,
                ).start()
            else:
                end = 0 if dz < 0 else 1
                pltpu.make_async_remote_copy(
                    src_ref=zsrc.at[r, end, from_x, from_y], dst_ref=zbuf.at[r, end, to_x, to_y],
                    send_sem=z_send.at[r], recv_sem=z_recv.at[r],
                    device_id=at(dx, dy, dz), device_id_type=MESH,
                ).start()

    def all_of(ref, sem):
        pltpu.make_async_copy(ref, ref, sem).wait()

    def share(stage, me, group, send_sem, recv_sem, k, value):
        stage[k, me] = value
        for peer in group:
            pltpu.make_async_remote_copy(
                src_ref=stage.at[k, me], dst_ref=stage.at[k, me],
                send_sem=send_sem.at[k], recv_sem=recv_sem.at[k],
                device_id=peer, device_id_type=MESH,
            ).start()

    def collect(stage, size, recv_sem, k):
        all_of(stage.at[k, pl.ds(0, size - 1)], recv_sem.at[k])
        return jnp.sum(stage[k], axis=0)

    def half_sum(value, width):
        while width < LANES:
            value = value + pltpu.roll(value, width, 1)
            width *= 2
        return value

    count = jnp.sum(state[WEIGHT], axis=0, keepdims=True)
    count = count + pltpu.roll(count, 64, 1)
    count = count + pltpu.roll(count, 32, 1)

    pl.semaphore_wait(barrier, len(peers))
    ship(0)

    def one_round(r, stretch):
        wide = jnp.broadcast_to(stretch, (8, LANES))
        half_step = jnp.where(r == 0, 0.0, 0.5 * TIME_STEP)
        here = state[WEIGHT] > 0.5
        position, velocity = [], []
        for k in range(3):
            position.append(state[BASE + k] + wide * state[TERM + k])
            velocity.append(wide * state[VEL + k] + (0.5 * TIME_STEP) * state[FORCE + k])
            state[POS + k] = position[k]
            for dz in (-1, 0, 1):
                moved = position[k] * (1.0 / UNIT)
                moved = pltpu.roll(moved, (SLOTS * dz) % LANES, 1) if dz else moved
                shifted[dz + 1, k] = moved - SIDE * dz if k == 2 else moved

        all_of(buf.at[r, pl.ds(0, 3)], halo_recv.at[r])
        all_of(zbuf.at[r], z_recv.at[r])

        narrow = wide[:1]
        for x in range(4):
            for y in range(4):
                lines[x * 4 + y, 0] = (buf[r, x, y, 0] + wide[:4] * buf[r, x, y, 1]) * (1.0 / UNIT)
                ends = [zbuf[r, e, x, y] for e in range(2)]
                ends = [e + narrow * pltpu.roll(e, LANES - SLOTS, 1) for e in ends]
                ends = jnp.where(cell[:1] % 2 == 0, ends[0], ends[1]) * (1.0 / UNIT)
                for k in range(3):
                    turned = pltpu.roll(ends, LANES - 2 * SLOTS * k, 1) if k else ends
                    lines[x * 4 + y, 1, k : k + 1, :] = turned
        for h in range(2):
            spread_lanes = cell * SLOTS + row + 8 * h
            for n in range(16):
                for k in range(3):
                    level, ghost = (
                        lane_take(jnp.broadcast_to(lines[n, e, k : k + 1, :], (8, LANES)), spread_lanes)
                        for e in range(2)
                    )
                    expand[n, 0, k, h] = jnp.where(cell == DEPTH - 1, ghost, level)
                    expand[n, 1, k, h] = level
                    expand[n, 2, k, h] = jnp.where(cell == 0, ghost, level)

        def one_column(c, carry):
            base = (c // 2) * 4 + c % 2
            total = [None] * 4
            for dz in (-1, 0, 1):
                own = [jnp.broadcast_to(shifted[dz + 1, k, pl.ds(c, 1), :], (8, LANES)) for k in range(3)]
                part = [jnp.zeros((8, LANES), jnp.float32)] * 4
                for dx in (-1, 0, 1):
                    own_x = own[0] - SIDE * dx
                    for dy in (-1, 0, 1):
                        own_y = own[1] - SIDE * dy
                        other = base + (dx + 1) * 4 + dy + 1
                        for h in range(2):
                            sx = expand[other, dz + 1, 0, h] - own_x
                            sy = expand[other, dz + 1, 1, h] - own_y
                            sz = expand[other, dz + 1, 2, h] - own[2]
                            squared = sx * sx + sy * sy + sz * sz
                            inside = squared < (CUTOFF / UNIT) ** 2
                            if (dx, dy, dz) == (0, 0, 0):
                                inside = inside & (slot != row + 8 * h)
                                squared = jnp.where(inside, squared, 1.0)
                            inverse_root = lax.rsqrt(squared)
                            inverse = inverse_root * inverse_root
                            six = inverse * inverse * inverse
                            wall = six * (six - 1.0)
                            strength = jnp.where(inside, wall * inverse - EDGE * inverse_root, 0.0)
                            energy = (wall - six) + (squared * inverse_root * (12.0 * EDGE) + ENERGY_SHIFT)
                            part[0] = part[0] + strength * sx
                            part[1] = part[1] + strength * sy
                            part[2] = part[2] + strength * sz
                            part[3] = part[3] + jnp.where(inside, energy, 0.0)
                for k in range(4):
                    back = pltpu.roll(part[k], (-SLOTS * dz) % LANES, 1) if dz else part[k]
                    total[k] = back if total[k] is None else total[k] + back
            for k in range(4):
                acc[k, c] = total[k]
            return carry

        lax.fori_loop(0, 4, one_column, 0, unroll=4)

        sums = []
        for k in range(4):
            for c in range(4):
                strip[c : c + 1, :] = jnp.sum(acc[k, c], axis=0, keepdims=True)
            sums.append(jnp.where(here & (row < 4), strip[...], 0.0))
        force, energy = [total * (-12.0 / UNIT) for total in sums[:3]], sums[3]
        vigor = jnp.zeros((8, LANES), jnp.float32)
        for k in range(3):
            velocity[k] = velocity[k] + half_step * force[k]
            vigor = vigor + velocity[k] * velocity[k]

        @pl.when(r > 0)
        def _():
            k_row = half_sum(jnp.sum(vigor, axis=0, keepdims=True), 64)
            u_row = half_sum(jnp.sum(energy, axis=0, keepdims=True), 32)
            n_row = count
            value = jnp.where(lane1 < 64, k_row, jnp.where(lane1 < 96, u_row, n_row))
            share(red_a, me_a, group_a, a_send, a_recv, r - 1, value)

        for k in range(3):
            state[VEL + k] = velocity[k]
            state[FORCE + k] = force[k]
            state[BASE + k] = position[k] + (0.5 * TIME_STEP * TIME_STEP) * force[k]
            state[TERM + k] = TIME_STEP * velocity[k]

        @pl.when(r < STEPS)
        def _():
            ship(r + 1)

        def reduced():
            value = collect(red_a, size_a, a_recv, r - 1)
            share(red_b, me_b, group_b, b_send, b_recv, r - 1, value)
            value = collect(red_b, size_b, b_recv, r - 1)
            vigor_sum = 0.5 * jnp.sum(jnp.where(lane1 < 64, value, 0.0), axis=1, keepdims=True)
            body_tally = jnp.sum(jnp.where(lane1 >= 96, value, 0.0), axis=1, keepdims=True)
            potential = 0.5 * jnp.sum(jnp.where((lane1 >= 64) & (lane1 < 96), value, 0.0), axis=1, keepdims=True)
            warmth = 2.0 * vigor_sum / (3.0 * body_tally)
            new = jnp.sqrt(1.0 + BATH_STRENGTH * (GOAL_WARMTH / warmth - 1.0))
            slot_total = float(nx * ny * nz * 4 * DEPTH * SLOTS)
            record = jnp.where(row == 0, potential, new * new * vigor_sum) / slot_total
            acc[4, 0] = jnp.where(lane == r - 1, record, acc[4, 0])
            return new

        return lax.cond(r > 0, reduced, lambda: jnp.ones((1, 1), jnp.float32))

    stretch = lax.fori_loop(0, ROUNDS, one_round, jnp.ones((1, 1), jnp.float32))

    for k in range(3):
        out_ref[k] = state[POS + k]
        out_ref[3 + k] = stretch * state[VEL + k]
        out_ref[6 + k] = state[FORCE + k]
    out_ref[9] = acc[4, 0]

    def drain(r, carry):
        all_of(buf.at[r, pl.ds(0, 3)], halo_send.at[r])
        all_of(zbuf.at[r], z_send.at[r])
        return carry

    lax.fori_loop(0, ROUNDS, drain, 0)

    def drain_sums(k, carry):
        all_of(red_a.at[k, pl.ds(0, size_a - 1)], a_send.at[k])
        all_of(red_b.at[k, pl.ds(0, size_b - 1)], b_send.at[k])
        return carry

    lax.fori_loop(0, STEPS, drain_sums, 0)


def unfold(in_ref, oo_ref, vo_ref, fo_ref, hist_ref):
    lane = lax.broadcasted_iota(jnp.int32, (8, LANES), 1)
    row = lax.broadcasted_iota(jnp.int32, (8, LANES), 0)
    lanes = row * SLOTS + lane % SLOTS
    for n, ref in enumerate((oo_ref, vo_ref, fo_ref)):
        for k in range(3):
            for c in range(4):
                line = jnp.broadcast_to(in_ref[3 * n + k, c : c + 1, :], (8, LANES))
                ref[c // 2, c % 2, k] = lane_take(line, lanes)[:, :SLOTS]
    hist_ref[...] = in_ref[9, :2, :STEPS]


def per_device(sizes, offsets, velocities, occupied):
    nx, ny, nz = sizes
    size_a, size_b = nz * 2, nx * (ny // 2)
    order = (0, 1, 4, 2, 3)
    block = jax.ShapeDtypeStruct((2, 2, 3, DEPTH, SLOTS), jnp.float32)
    whole = pl.BlockSpec(memory_space=pltpu.VMEM)
    dma = pltpu.SemaphoreType.DMA
    vmem = functools.partial(lambda *shape: pltpu.VMEM(shape, jnp.float32))
    lines = pl.pallas_call(
        functools.partial(kernel, sizes),
        out_shape=pltpu.VMEM((10, 8, LANES), jnp.float32),
        in_specs=[pl.BlockSpec(memory_space=pl.ANY)] * 3,
        out_specs=whole,
        scratch_shapes=[
            vmem(2, 2, 3, DEPTH, SLOTS), vmem(2, 2, 3, DEPTH, SLOTS), pltpu.VMEM((2, 2, DEPTH, SLOTS), jnp.int32), dma((3,)),
            vmem(ROUNDS, 4, 4, 2, 4, LANES),
            vmem(ROUNDS, 2, 2, 2, 1, LANES),
            vmem(ROUNDS, 2, 4, 4, 1, LANES),
            vmem(STEPS, size_a, 1, LANES),
            vmem(STEPS, size_b, 1, LANES),
            vmem(16, 2, 4, LANES),
            vmem(16, 3, 3, 2, 8, LANES),
            vmem(5, 4, 8, LANES),
            vmem(16, 8, LANES),
            vmem(3, 3, 8, LANES),
            vmem(8, LANES),
            dma((ROUNDS,)), dma((ROUNDS,)), dma((ROUNDS,)), dma((ROUNDS,)),
            dma((STEPS,)), dma((STEPS,)), dma((STEPS,)), dma((STEPS,)),
        ],
        compiler_params=pltpu.CompilerParams(collective_id=0, has_side_effects=True),
        name="window",
    )(offsets.transpose(order), velocities.transpose(order), occupied)
    position, velocity, force, history = pl.pallas_call(
        unfold,
        out_shape=(block, block, block, jax.ShapeDtypeStruct((2, STEPS), jnp.float32)),
        in_specs=[whole],
        out_specs=(whole,) * 4,
        name="unfold",
    )(pltpu.with_memory_space_constraint(lines, pltpu.VMEM))
    back = (0, 1, 3, 4, 2)
    return (position.transpose(back), velocity.transpose(back), force.transpose(back), history.T)


def solution(mesh):
    sizes = tuple(mesh.shape[a] for a in ("gx", "gy", "gz"))
    cells = P("gx", "gy", "gz", None, None)
    return jax.shard_map(
        functools.partial(per_device, sizes),
        mesh=mesh,
        in_specs=(cells, cells, P("gx", "gy", "gz", None)),
        out_specs=(cells, cells, cells, P()),
        check_vma=False,
    )
```

```python
import functools
import itertools

import jax
import jax.numpy as jnp
from jax import lax
from jax.experimental import pallas as pl
from jax.experimental.pallas import tpu as pltpu
from jax.sharding import PartitionSpec as P

STEPS = 4
ROUNDS = STEPS + 1
CUTOFF = 2.5
CELL_SIDE = 2.6
TIME_STEP = 0.005
BATH_STRENGTH = 0.25
GOAL_WARMTH = 0.8
FORCE_EDGE = 24.0 * (2.0 * CUTOFF ** (-13) - CUTOFF ** (-7))
ENERGY_EDGE = 4.0 * (CUTOFF ** (-12) - CUTOFF ** (-6))
ENERGY_SHIFT = -ENERGY_EDGE - CUTOFF * FORCE_EDGE
UNIT = 2.0 ** (1.0 / 6.0)
SIDE = CELL_SIDE / UNIT
EDGE = FORCE_EDGE * UNIT / 12.0
REACH = (CUTOFF / UNIT) ** 2
FAR = 64.0
MESH = pl.DeviceIdType.MESH
LANES = 128
SLOTS = 16
DEPTH = 8

SIDES = {0: (pl.ds(0, 2), pl.ds(1, 2)), 1: (pl.ds(1, 1), pl.ds(0, 1)), -1: (pl.ds(0, 1), pl.ds(3, 1))}
NEIGHBOURS = sorted(
    (d for d in itertools.product((-1, 0, 1), repeat=3) if d != (0, 0, 0)),
    key=lambda d: -(2 * abs(d[0]) + 2 * abs(d[1]) + abs(d[2])),
)


def lane_take(x, lanes):
    return jnp.take_along_axis(x, lanes, axis=1, mode="promise_in_bounds")


def kernel(
    sizes, o_hbm, v_hbm, w_hbm, out_ref, o_ref, v_ref, w_ref, in_sem,
    buf, zsrc, zbuf, red_a, red_b, lines, expand, acc, state, shifted, strip,
    halo_recv, halo_send, z_recv, z_send, a_recv, a_send, b_recv, b_send,
):
    nx, ny, nz = sizes
    gx, gy, gz = (lax.axis_index(a) for a in ("gx", "gy", "gz"))
    high, core = gy // 2, gy % 2
    n_high = ny // 2

    def at(dx, dy, dz):
        return (lax.rem(gx + dx + nx, nx), lax.rem(gy + dy + ny, ny), lax.rem(gz + dz + nz, nz))

    group_a = [
        (gx, high * 2 + lax.rem(core + dc, 2), lax.rem(gz + dz, nz))
        for dz in range(nz) for dc in range(2) if (dz, dc) != (0, 0)
    ]
    me_a = gz * 2 + core
    group_b = [
        (lax.rem(gx + dx, nx), lax.rem(high + dh, n_high) * 2 + core, gz)
        for dx in range(nx) for dh in range(n_high) if (dx, dh) != (0, 0)
    ]
    me_b = gx * n_high + high
    size_a, size_b = nz * 2, nx * n_high

    barrier = pltpu.get_barrier_semaphore()
    peers = [at(*d) for d in NEIGHBOURS] + group_a + group_b
    for peer in peers:
        pl.semaphore_signal(barrier, inc=1, device_id=peer, device_id_type=MESH)

    fetches = [
        pltpu.make_async_copy(src, dst, in_sem.at[n])
        for n, (src, dst) in enumerate(((o_hbm, o_ref), (v_hbm, v_ref), (w_hbm, w_ref)))
    ]
    for fetch in fetches:
        fetch.start()

    lane = lax.broadcasted_iota(jnp.int32, (8, LANES), 1)
    row = lax.broadcasted_iota(jnp.int32, (8, LANES), 0)
    slot, cell = lane % SLOTS, lane // SLOTS
    lane1 = lane[:1]

    def flatten(n, block):
        expand[n // 18, n // 6 % 3, n // 2 % 3, n % 2, :, :SLOTS] = block
        spread = lane_take(expand[n // 18, n // 6 % 3, n // 2 % 3, n % 2], slot)
        return jnp.sum(jnp.where(cell == row, spread, 0.0), axis=0, keepdims=True)

    for k in range(16):
        state[k] = jnp.zeros((8, LANES), jnp.float32)
    POS, VEL, FORCE, BASE, TERM, WEIGHT = 0, 3, 6, 9, 12, 15
    for fetch in fetches:
        fetch.wait()
    for c in range(4):
        cx, cy = c // 2, c % 2
        state[WEIGHT, c : c + 1, :] = flatten(7 * c, w_ref[cx, cy].astype(jnp.float32))
        for k in range(3):
            state[BASE + k, c : c + 1, :] = flatten(7 * c + 1 + k, o_ref[cx, cy, k])
            state[VEL + k, c : c + 1, :] = flatten(7 * c + 4 + k, v_ref[cx, cy, k])
    for k in range(3):
        state[VEL + k] = state[VEL + k] * state[WEIGHT]
    acc[...] = jnp.zeros_like(acc)
    for r in range(ROUNDS):
        for cx in range(2):
            for cy in range(2):
                buf[r, 1 + cx, 1 + cy] = jnp.zeros((2, 4, LANES), jnp.float32)

    def ship(r):
        here = state[WEIGHT] > 0.5
        base = [jnp.where(here, state[BASE + k], FAR) for k in range(3)]
        term = [state[TERM + k] for k in range(3)]
        for c in range(4):
            for k in range(3):
                buf[r, 1 + c // 2, 1 + c % 2, 0, k : k + 1, :] = base[k][c : c + 1]
                buf[r, 1 + c // 2, 1 + c % 2, 1, k : k + 1, :] = term[k][c : c + 1]
        for end in range(2):
            pick = slot + end * (LANES - SLOTS)
            packed = jnp.zeros((8, LANES), jnp.float32)
            for k in range(3):
                place = (2 * k + (DEPTH - 1) * end) % DEPTH
                packed = jnp.where(cell == place, lane_take(base[k], pick), packed)
                packed = jnp.where(cell == (place + 1) % DEPTH, lane_take(term[k], pick), packed)
            for c in range(4):
                zsrc[r, end, c // 2, c % 2] = packed[c : c + 1]
        for dx, dy, dz in NEIGHBOURS:
            (from_x, to_x), (from_y, to_y) = SIDES[dx], SIDES[dy]
            if dz == 0:
                own_x, own_y = pl.ds(from_x.start + 1, from_x.size), pl.ds(from_y.start + 1, from_y.size)
                pltpu.make_async_remote_copy(
                    src_ref=buf.at[r, own_x, own_y], dst_ref=buf.at[r, to_x, to_y],
                    send_sem=halo_send.at[r], recv_sem=halo_recv.at[r],
                    device_id=at(dx, dy, dz), device_id_type=MESH,
                ).start()
            else:
                end = 0 if dz < 0 else 1
                pltpu.make_async_remote_copy(
                    src_ref=zsrc.at[r, end, from_x, from_y], dst_ref=zbuf.at[r, end, to_x, to_y],
                    send_sem=z_send.at[r], recv_sem=z_recv.at[r],
                    device_id=at(dx, dy, dz), device_id_type=MESH,
                ).start()

    def all_of(ref, sem):
        pltpu.make_async_copy(ref, ref, sem).wait()

    def share(stage, me, group, send_sem, recv_sem, k, value):
        stage[k, me] = value
        for peer in group:
            pltpu.make_async_remote_copy(
                src_ref=stage.at[k, me], dst_ref=stage.at[k, me],
                send_sem=send_sem.at[k], recv_sem=recv_sem.at[k],
                device_id=peer, device_id_type=MESH,
            ).start()

    def collect(stage, size, recv_sem, k):
        all_of(stage.at[k, pl.ds(0, size - 1)], recv_sem.at[k])
        return jnp.sum(stage[k], axis=0)

    def half_sum(value, width):
        while width < LANES:
            value = value + pltpu.roll(value, width, 1)
            width *= 2
        return value

    count = jnp.sum(state[WEIGHT], axis=0, keepdims=True)
    count = count + pltpu.roll(count, 64, 1)
    count = count + pltpu.roll(count, 32, 1)

    pl.semaphore_wait(barrier, len(peers))
    ship(0)

    def one_round(r, stretch):
        wide = jnp.broadcast_to(stretch, (8, LANES))
        half_step = jnp.where(r == 0, 0.0, 0.5 * TIME_STEP)
        here = state[WEIGHT] > 0.5
        position, velocity = [], []
        for k in range(3):
            position.append(state[BASE + k] + wide * state[TERM + k])
            velocity.append(wide * state[VEL + k] + (0.5 * TIME_STEP) * state[FORCE + k])
            state[POS + k] = position[k]
            for dz in (-1, 0, 1):
                moved = position[k] * (1.0 / UNIT)
                moved = pltpu.roll(moved, (SLOTS * dz) % LANES, 1) if dz else moved
                shifted[dz + 1, k] = moved - SIDE * dz if k == 2 else moved

        all_of(buf.at[r, pl.ds(0, 3)], halo_recv.at[r])
        all_of(zbuf.at[r], z_recv.at[r])

        narrow = wide[:1]
        for x in range(4):
            for y in range(4):
                lines[x * 4 + y, 0] = (buf[r, x, y, 0] + wide[:4] * buf[r, x, y, 1]) * (1.0 / UNIT)
                ends = [zbuf[r, e, x, y] for e in range(2)]
                ends = [e + narrow * pltpu.roll(e, LANES - SLOTS, 1) for e in ends]
                ends = jnp.where(cell[:1] % 2 == 0, ends[0], ends[1]) * (1.0 / UNIT)
                for k in range(3):
                    turned = pltpu.roll(ends, LANES - 2 * SLOTS * k, 1) if k else ends
                    lines[x * 4 + y, 1, k : k + 1, :] = turned
        for h in range(2):
            spread_lanes = cell * SLOTS + row + 8 * h
            for n in range(16):
                for k in range(3):
                    level, ghost = (
                        lane_take(jnp.broadcast_to(lines[n, e, k : k + 1, :], (8, LANES)), spread_lanes)
                        for e in range(2)
                    )
                    expand[n, 0, k, h] = jnp.where(cell == DEPTH - 1, ghost, level)
                    expand[n, 1, k, h] = level
                    expand[n, 2, k, h] = jnp.where(cell == 0, ghost, level)

        def one_column(c, carry):
            base = (c // 2) * 4 + c % 2
            total = [None] * 4
            for dz in (-1, 0, 1):
                own = [jnp.broadcast_to(shifted[dz + 1, k, pl.ds(c, 1), :], (8, LANES)) for k in range(3)]
                part = [jnp.zeros((8, LANES), jnp.float32)] * 4
                distance = part[0]
                for dx in (-1, 0, 1):
                    own_x = own[0] - SIDE * dx
                    for dy in (-1, 0, 1):
                        own_y = own[1] - SIDE * dy
                        other = base + (dx + 1) * 4 + dy + 1
                        for h in range(2):
                            sx = expand[other, dz + 1, 0, h] - own_x
                            sy = expand[other, dz + 1, 1, h] - own_y
                            sz = expand[other, dz + 1, 2, h] - own[2]
                            squared = sx * sx + sy * sy + sz * sz
                            if (dx, dy, dz) == (0, 0, 0):
                                squared = jnp.where(slot == row + 8 * h, REACH, squared)
                            squared = jnp.minimum(squared, REACH)
                            inverse_root = lax.rsqrt(squared)
                            inverse = inverse_root * inverse_root
                            six = inverse * inverse * inverse
                            wall = six * (six - 1.0)
                            strength = wall * inverse - EDGE * inverse_root
                            part[0] = part[0] + strength * sx
                            part[1] = part[1] + strength * sy
                            part[2] = part[2] + strength * sz
                            part[3] = part[3] + (wall - six)
                            distance = distance + squared * inverse_root
                part[3] = part[3] + (12.0 * EDGE) * distance + 18.0 * ENERGY_SHIFT
                for k in range(4):
                    back = pltpu.roll(part[k], (-SLOTS * dz) % LANES, 1) if dz else part[k]
                    total[k] = back if total[k] is None else total[k] + back
            for k in range(4):
                acc[k, c] = total[k]
            return carry

        lax.fori_loop(0, 4, one_column, 0, unroll=4)

        sums = []
        for k in range(4):
            for c in range(4):
                strip[c : c + 1, :] = jnp.sum(acc[k, c], axis=0, keepdims=True)
            sums.append(jnp.where(here & (row < 4), strip[...], 0.0))
        force, energy = [total * (-12.0 / UNIT) for total in sums[:3]], sums[3]
        vigor = jnp.zeros((8, LANES), jnp.float32)
        for k in range(3):
            velocity[k] = velocity[k] + half_step * force[k]
            vigor = vigor + velocity[k] * velocity[k]

        @pl.when(r > 0)
        def _():
            k_row = half_sum(jnp.sum(vigor, axis=0, keepdims=True), 64)
            u_row = half_sum(jnp.sum(energy, axis=0, keepdims=True), 32)
            n_row = count
            value = jnp.where(lane1 < 64, k_row, jnp.where(lane1 < 96, u_row, n_row))
            share(red_a, me_a, group_a, a_send, a_recv, r - 1, value)

        for k in range(3):
            state[VEL + k] = velocity[k]
            state[FORCE + k] = force[k]
            state[BASE + k] = position[k] + (0.5 * TIME_STEP * TIME_STEP) * force[k]
            state[TERM + k] = TIME_STEP * velocity[k]

        @pl.when(r < STEPS)
        def _():
            ship(r + 1)

        def reduced():
            value = collect(red_a, size_a, a_recv, r - 1)
            share(red_b, me_b, group_b, b_send, b_recv, r - 1, value)
            value = collect(red_b, size_b, b_recv, r - 1)
            vigor_sum = 0.5 * jnp.sum(jnp.where(lane1 < 64, value, 0.0), axis=1, keepdims=True)
            body_tally = jnp.sum(jnp.where(lane1 >= 96, value, 0.0), axis=1, keepdims=True)
            potential = 0.5 * jnp.sum(jnp.where((lane1 >= 64) & (lane1 < 96), value, 0.0), axis=1, keepdims=True)
            warmth = 2.0 * vigor_sum / (3.0 * body_tally)
            new = jnp.sqrt(1.0 + BATH_STRENGTH * (GOAL_WARMTH / warmth - 1.0))
            slot_total = float(nx * ny * nz * 4 * DEPTH * SLOTS)
            record = jnp.where(row == 0, potential, new * new * vigor_sum) / slot_total
            acc[4, 0] = jnp.where(lane == r - 1, record, acc[4, 0])
            return new

        return lax.cond(r > 0, reduced, lambda: jnp.ones((1, 1), jnp.float32))

    stretch = lax.fori_loop(0, ROUNDS, one_round, jnp.ones((1, 1), jnp.float32))

    for k in range(3):
        out_ref[k] = state[POS + k]
        out_ref[3 + k] = stretch * state[VEL + k]
        out_ref[6 + k] = state[FORCE + k]
    out_ref[9] = acc[4, 0]

    def drain(r, carry):
        all_of(buf.at[r, pl.ds(0, 3)], halo_send.at[r])
        all_of(zbuf.at[r], z_send.at[r])
        return carry

    lax.fori_loop(0, ROUNDS, drain, 0)

    def drain_sums(k, carry):
        all_of(red_a.at[k, pl.ds(0, size_a - 1)], a_send.at[k])
        all_of(red_b.at[k, pl.ds(0, size_b - 1)], b_send.at[k])
        return carry

    lax.fori_loop(0, STEPS, drain_sums, 0)


def unfold(in_ref, oo_ref, vo_ref, fo_ref, hist_ref):
    lane = lax.broadcasted_iota(jnp.int32, (8, LANES), 1)
    row = lax.broadcasted_iota(jnp.int32, (8, LANES), 0)
    lanes = row * SLOTS + lane % SLOTS
    for n, ref in enumerate((oo_ref, vo_ref, fo_ref)):
        for k in range(3):
            for c in range(4):
                line = jnp.broadcast_to(in_ref[3 * n + k, c : c + 1, :], (8, LANES))
                ref[c // 2, c % 2, k] = lane_take(line, lanes)[:, :SLOTS]
    hist_ref[...] = in_ref[9, :2, :STEPS]


def per_device(sizes, offsets, velocities, occupied):
    nx, ny, nz = sizes
    size_a, size_b = nz * 2, nx * (ny // 2)
    order = (0, 1, 4, 2, 3)
    block = jax.ShapeDtypeStruct((2, 2, 3, DEPTH, SLOTS), jnp.float32)
    whole = pl.BlockSpec(memory_space=pltpu.VMEM)
    dma = pltpu.SemaphoreType.DMA
    vmem = functools.partial(lambda *shape: pltpu.VMEM(shape, jnp.float32))
    lines = pl.pallas_call(
        functools.partial(kernel, sizes),
        out_shape=pltpu.VMEM((10, 8, LANES), jnp.float32),
        in_specs=[pl.BlockSpec(memory_space=pl.ANY)] * 3,
        out_specs=whole,
        scratch_shapes=[
            vmem(2, 2, 3, DEPTH, SLOTS), vmem(2, 2, 3, DEPTH, SLOTS), pltpu.VMEM((2, 2, DEPTH, SLOTS), jnp.int32), dma((3,)),
            vmem(ROUNDS, 4, 4, 2, 4, LANES),
            vmem(ROUNDS, 2, 2, 2, 1, LANES),
            vmem(ROUNDS, 2, 4, 4, 1, LANES),
            vmem(STEPS, size_a, 1, LANES),
            vmem(STEPS, size_b, 1, LANES),
            vmem(16, 2, 4, LANES),
            vmem(16, 3, 3, 2, 8, LANES),
            vmem(5, 4, 8, LANES),
            vmem(16, 8, LANES),
            vmem(3, 3, 8, LANES),
            vmem(8, LANES),
            dma((ROUNDS,)), dma((ROUNDS,)), dma((ROUNDS,)), dma((ROUNDS,)),
            dma((STEPS,)), dma((STEPS,)), dma((STEPS,)), dma((STEPS,)),
        ],
        compiler_params=pltpu.CompilerParams(collective_id=0, has_side_effects=True),
        name="window",
    )(offsets.transpose(order), velocities.transpose(order), occupied)
    position, velocity, force, history = pl.pallas_call(
        unfold,
        out_shape=(block, block, block, jax.ShapeDtypeStruct((2, STEPS), jnp.float32)),
        in_specs=[whole],
        out_specs=(whole,) * 4,
        name="unfold",
    )(pltpu.with_memory_space_constraint(lines, pltpu.VMEM))
    back = (0, 1, 3, 4, 2)
    return (position.transpose(back), velocity.transpose(back), force.transpose(back), history.T)


def solution(mesh):
    sizes = tuple(mesh.shape[a] for a in ("gx", "gy", "gz"))
    cells = P("gx", "gy", "gz", None, None)
    return jax.shard_map(
        functools.partial(per_device, sizes),
        mesh=mesh,
        in_specs=(cells, cells, P("gx", "gy", "gz", None)),
        out_specs=(cells, cells, cells, P()),
        check_vma=False,
    )
```

```python
import functools
import itertools

import jax
import jax.numpy as jnp
from jax import lax
from jax.experimental import pallas as pl
from jax.experimental.pallas import tpu as pltpu
from jax.sharding import PartitionSpec as P

STEPS = 4
ROUNDS = STEPS + 1
CUTOFF = 2.5
CELL_SIDE = 2.6
TIME_STEP = 0.005
BATH_STRENGTH = 0.25
GOAL_WARMTH = 0.8
FORCE_EDGE = 24.0 * (2.0 * CUTOFF ** (-13) - CUTOFF ** (-7))
ENERGY_EDGE = 4.0 * (CUTOFF ** (-12) - CUTOFF ** (-6))
ENERGY_SHIFT = -ENERGY_EDGE - CUTOFF * FORCE_EDGE
UNIT = 2.0 ** (1.0 / 6.0)
SIDE = CELL_SIDE / UNIT
EDGE = FORCE_EDGE * UNIT / 12.0
REACH = (CUTOFF / UNIT) ** 2
FAR = 64.0
MESH = pl.DeviceIdType.MESH
LANES = 128
SLOTS = 16
DEPTH = 8

SIDES = {0: (pl.ds(0, 2), pl.ds(1, 2)), 1: (pl.ds(1, 1), pl.ds(0, 1)), -1: (pl.ds(0, 1), pl.ds(3, 1))}
NEIGHBOURS = sorted(
    (d for d in itertools.product((-1, 0, 1), repeat=3) if d != (0, 0, 0)),
    key=lambda d: -(2 * abs(d[0]) + 2 * abs(d[1]) + abs(d[2])),
)


def lane_take(x, lanes):
    return jnp.take_along_axis(x, lanes, axis=1, mode="promise_in_bounds")


def kernel(
    sizes, o_hbm, v_hbm, w_hbm, out_ref, o_ref, v_ref, w_ref, in_sem,
    buf, zsrc, zbuf, red_a, red_b, lines, expand, acc, state, shifted, strip,
    halo_recv, halo_send, z_recv, z_send, a_recv, a_send, b_recv, b_send,
):
    nx, ny, nz = sizes
    gx, gy, gz = (lax.axis_index(a) for a in ("gx", "gy", "gz"))
    high, core = gy // 2, gy % 2
    n_high = ny // 2

    def at(dx, dy, dz):
        return (lax.rem(gx + dx + nx, nx), lax.rem(gy + dy + ny, ny), lax.rem(gz + dz + nz, nz))

    group_a = [
        (gx, high * 2 + lax.rem(core + dc, 2), lax.rem(gz + dz, nz))
        for dz in range(nz) for dc in range(2) if (dz, dc) != (0, 0)
    ]
    me_a = gz * 2 + core
    group_b = [
        (lax.rem(gx + dx, nx), lax.rem(high + dh, n_high) * 2 + core, gz)
        for dx in range(nx) for dh in range(n_high) if (dx, dh) != (0, 0)
    ]
    me_b = gx * n_high + high
    size_a, size_b = nz * 2, nx * n_high

    barrier = pltpu.get_barrier_semaphore()
    peers = [at(*d) for d in NEIGHBOURS] + group_a + group_b
    for peer in peers:
        pl.semaphore_signal(barrier, inc=1, device_id=peer, device_id_type=MESH)

    fetches = [
        pltpu.make_async_copy(src, dst, in_sem.at[n])
        for n, (src, dst) in enumerate(((o_hbm, o_ref), (v_hbm, v_ref), (w_hbm, w_ref)))
    ]
    for fetch in fetches:
        fetch.start()

    lane = lax.broadcasted_iota(jnp.int32, (8, LANES), 1)
    row = lax.broadcasted_iota(jnp.int32, (8, LANES), 0)
    slot, cell = lane % SLOTS, lane // SLOTS
    lane1 = lane[:1]

    def flatten(n, block):
        expand[n // 18, n // 6 % 3, n // 2 % 3, n % 2, :, :SLOTS] = block
        spread = lane_take(expand[n // 18, n // 6 % 3, n // 2 % 3, n % 2], slot)
        return jnp.sum(jnp.where(cell == row, spread, 0.0), axis=0, keepdims=True)

    for k in range(16):
        state[k] = jnp.zeros((8, LANES), jnp.float32)
    POS, VEL, FORCE, BASE, TERM, WEIGHT = 0, 3, 6, 9, 12, 15
    for fetch in fetches:
        fetch.wait()
    for c in range(4):
        cx, cy = c // 2, c % 2
        state[WEIGHT, c : c + 1, :] = flatten(7 * c, w_ref[cx, cy].astype(jnp.float32))
        for k in range(3):
            state[BASE + k, c : c + 1, :] = flatten(7 * c + 1 + k, o_ref[cx, cy, k])
            state[VEL + k, c : c + 1, :] = flatten(7 * c + 4 + k, v_ref[cx, cy, k])
    for k in range(3):
        state[VEL + k] = state[VEL + k] * state[WEIGHT]
    acc[...] = jnp.zeros_like(acc)
    for r in range(ROUNDS):
        for cx in range(2):
            for cy in range(2):
                buf[r, 1 + cx, 1 + cy] = jnp.zeros((2, 4, LANES), jnp.float32)

    def ship(r):
        here = state[WEIGHT] > 0.5
        base = [jnp.where(here, state[BASE + k], FAR) for k in range(3)]
        term = [state[TERM + k] for k in range(3)]
        for c in range(4):
            for k in range(3):
                buf[r, 1 + c // 2, 1 + c % 2, 0, k : k + 1, :] = base[k][c : c + 1]
                buf[r, 1 + c // 2, 1 + c % 2, 1, k : k + 1, :] = term[k][c : c + 1]
        for end in range(2):
            pick = slot + end * (LANES - SLOTS)
            packed = jnp.zeros((8, LANES), jnp.float32)
            for k in range(3):
                place = (2 * k + (DEPTH - 1) * end) % DEPTH
                packed = jnp.where(cell == place, lane_take(base[k], pick), packed)
                packed = jnp.where(cell == (place + 1) % DEPTH, lane_take(term[k], pick), packed)
            for c in range(4):
                zsrc[r, end, c // 2, c % 2] = packed[c : c + 1]
        for dx, dy, dz in NEIGHBOURS:
            (from_x, to_x), (from_y, to_y) = SIDES[dx], SIDES[dy]
            if dz == 0:
                own_x, own_y = pl.ds(from_x.start + 1, from_x.size), pl.ds(from_y.start + 1, from_y.size)
                pltpu.make_async_remote_copy(
                    src_ref=buf.at[r, own_x, own_y], dst_ref=buf.at[r, to_x, to_y],
                    send_sem=halo_send.at[r], recv_sem=halo_recv.at[r],
                    device_id=at(dx, dy, dz), device_id_type=MESH,
                ).start()
            else:
                end = 0 if dz < 0 else 1
                pltpu.make_async_remote_copy(
                    src_ref=zsrc.at[r, end, from_x, from_y], dst_ref=zbuf.at[r, end, to_x, to_y],
                    send_sem=z_send.at[r], recv_sem=z_recv.at[r],
                    device_id=at(dx, dy, dz), device_id_type=MESH,
                ).start()

    def all_of(ref, sem):
        pltpu.make_async_copy(ref, ref, sem).wait()

    def share(stage, me, group, send_sem, recv_sem, k, value):
        stage[k, me] = value
        for peer in group:
            pltpu.make_async_remote_copy(
                src_ref=stage.at[k, me], dst_ref=stage.at[k, me],
                send_sem=send_sem.at[k], recv_sem=recv_sem.at[k],
                device_id=peer, device_id_type=MESH,
            ).start()

    def collect(stage, size, recv_sem, k):
        all_of(stage.at[k, pl.ds(0, size - 1)], recv_sem.at[k])
        return jnp.sum(stage[k], axis=0)

    def half_sum(value, width):
        while width < LANES:
            value = value + pltpu.roll(value, width, 1)
            width *= 2
        return value

    count = jnp.sum(state[WEIGHT], axis=0, keepdims=True)
    count = count + pltpu.roll(count, 64, 1)
    count = count + pltpu.roll(count, 32, 1)

    pl.semaphore_wait(barrier, len(peers))
    ship(0)

    def one_round(r, stretch):
        wide = jnp.broadcast_to(stretch, (8, LANES))
        half_step = jnp.where(r == 0, 0.0, 0.5 * TIME_STEP)
        here = state[WEIGHT] > 0.5
        position, velocity = [], []
        for k in range(3):
            position.append(state[BASE + k] + wide * state[TERM + k])
            velocity.append(wide * state[VEL + k] + (0.5 * TIME_STEP) * state[FORCE + k])
            state[POS + k] = position[k]
            for dz in (-1, 0, 1):
                moved = position[k] * (1.0 / UNIT)
                moved = pltpu.roll(moved, (SLOTS * dz) % LANES, 1) if dz else moved
                shifted[dz + 1, k] = moved - SIDE * dz if k == 2 else moved

        all_of(buf.at[r, pl.ds(0, 3)], halo_recv.at[r])
        all_of(zbuf.at[r], z_recv.at[r])

        narrow = wide[:1]
        for x in range(4):
            for y in range(4):
                lines[x * 4 + y, 0] = (buf[r, x, y, 0] + wide[:4] * buf[r, x, y, 1]) * (1.0 / UNIT)
                ends = [zbuf[r, e, x, y] for e in range(2)]
                ends = [e + narrow * pltpu.roll(e, LANES - SLOTS, 1) for e in ends]
                ends = jnp.where(cell[:1] % 2 == 0, ends[0], ends[1]) * (1.0 / UNIT)
                for k in range(3):
                    turned = pltpu.roll(ends, LANES - 2 * SLOTS * k, 1) if k else ends
                    lines[x * 4 + y, 1, k : k + 1, :] = turned
        for h in range(2):
            spread_lanes = cell * SLOTS + row + 8 * h
            for n in range(16):
                for k in range(3):
                    level, ghost = (
                        lane_take(jnp.broadcast_to(lines[n, e, k : k + 1, :], (8, LANES)), spread_lanes)
                        for e in range(2)
                    )
                    expand[n, 0, k, h] = jnp.where(cell == DEPTH - 1, ghost, level)
                    expand[n, 1, k, h] = level
                    expand[n, 2, k, h] = jnp.where(cell == 0, ghost, level)

        def one_column(c, carry):
            base = (c // 2) * 4 + c % 2
            total = [None] * 4
            for dz in (-1, 0, 1):
                own = [jnp.broadcast_to(shifted[dz + 1, k, pl.ds(c, 1), :], (8, LANES)) for k in range(3)]
                part = [jnp.zeros((8, LANES), jnp.float32)] * 4
                distance = part[0]
                for dx in (-1, 0, 1):
                    own_x = own[0] - SIDE * dx
                    for dy in (-1, 0, 1):
                        own_y = own[1] - SIDE * dy
                        other = base + (dx + 1) * 4 + dy + 1
                        for h in range(2):
                            sx = expand[other, dz + 1, 0, h] - own_x
                            sy = expand[other, dz + 1, 1, h] - own_y
                            sz = expand[other, dz + 1, 2, h] - own[2]
                            squared = sx * sx + sy * sy + sz * sz
                            if (dx, dy, dz) == (0, 0, 0):
                                squared = jnp.where(slot == row + 8 * h, REACH, squared)
                            squared = jnp.minimum(squared, REACH)
                            inverse_root = lax.rsqrt(squared)
                            inverse = inverse_root * inverse_root
                            six = inverse * inverse * inverse
                            wall = six * (six - 1.0)
                            strength = wall * inverse - EDGE * inverse_root
                            part[0] = part[0] + strength * sx
                            part[1] = part[1] + strength * sy
                            part[2] = part[2] + strength * sz
                            part[3] = part[3] + (wall - six)
                            distance = distance + squared * inverse_root
                part[3] = part[3] + (12.0 * EDGE) * distance + 18.0 * ENERGY_SHIFT
                for k in range(4):
                    back = pltpu.roll(part[k], (-SLOTS * dz) % LANES, 1) if dz else part[k]
                    total[k] = back if total[k] is None else total[k] + back
            for k in range(4):
                acc[k, c] = total[k]
            return carry

        lax.fori_loop(0, 4, one_column, 0, unroll=4)

        sums = []
        for k in range(4):
            for c in range(4):
                strip[k, c : c + 1, :] = jnp.sum(acc[k, c], axis=0, keepdims=True)
        for k in range(4):
            sums.append(jnp.where(here & (row < 4), strip[k], 0.0))
        force, energy = [total * (-12.0 / UNIT) for total in sums[:3]], sums[3]
        vigor = jnp.zeros((8, LANES), jnp.float32)
        for k in range(3):
            velocity[k] = velocity[k] + half_step * force[k]
            vigor = vigor + velocity[k] * velocity[k]

        @pl.when(r > 0)
        def _():
            k_row = half_sum(jnp.sum(vigor, axis=0, keepdims=True), 64)
            u_row = half_sum(jnp.sum(energy, axis=0, keepdims=True), 32)
            n_row = count
            value = jnp.where(lane1 < 64, k_row, jnp.where(lane1 < 96, u_row, n_row))
            share(red_a, me_a, group_a, a_send, a_recv, r - 1, value)

        for k in range(3):
            state[VEL + k] = velocity[k]
            state[FORCE + k] = force[k]
            state[BASE + k] = position[k] + (0.5 * TIME_STEP * TIME_STEP) * force[k]
            state[TERM + k] = TIME_STEP * velocity[k]

        @pl.when(r < STEPS)
        def _():
            ship(r + 1)

        def reduced():
            value = collect(red_a, size_a, a_recv, r - 1)
            share(red_b, me_b, group_b, b_send, b_recv, r - 1, value)
            value = collect(red_b, size_b, b_recv, r - 1)
            vigor_sum = 0.5 * jnp.sum(jnp.where(lane1 < 64, value, 0.0), axis=1, keepdims=True)
            body_tally = jnp.sum(jnp.where(lane1 >= 96, value, 0.0), axis=1, keepdims=True)
            potential = 0.5 * jnp.sum(jnp.where((lane1 >= 64) & (lane1 < 96), value, 0.0), axis=1, keepdims=True)
            warmth = 2.0 * vigor_sum / (3.0 * body_tally)
            new = jnp.sqrt(1.0 + BATH_STRENGTH * (GOAL_WARMTH / warmth - 1.0))
            slot_total = float(nx * ny * nz * 4 * DEPTH * SLOTS)
            record = jnp.where(row == 0, potential, new * new * vigor_sum) / slot_total
            acc[4, 0] = jnp.where(lane == r - 1, record, acc[4, 0])
            return new

        return lax.cond(r > 0, reduced, lambda: jnp.ones((1, 1), jnp.float32))

    stretch = lax.fori_loop(0, ROUNDS, one_round, jnp.ones((1, 1), jnp.float32))

    for k in range(3):
        out_ref[k] = state[POS + k]
        out_ref[3 + k] = stretch * state[VEL + k]
        out_ref[6 + k] = state[FORCE + k]
    out_ref[9] = acc[4, 0]

    def drain(r, carry):
        all_of(buf.at[r, pl.ds(0, 3)], halo_send.at[r])
        all_of(zbuf.at[r], z_send.at[r])
        return carry

    lax.fori_loop(0, ROUNDS, drain, 0)

    def drain_sums(k, carry):
        all_of(red_a.at[k, pl.ds(0, size_a - 1)], a_send.at[k])
        all_of(red_b.at[k, pl.ds(0, size_b - 1)], b_send.at[k])
        return carry

    lax.fori_loop(0, STEPS, drain_sums, 0)


def unfold(in_ref, oo_ref, vo_ref, fo_ref, hist_ref):
    lane = lax.broadcasted_iota(jnp.int32, (8, LANES), 1)
    row = lax.broadcasted_iota(jnp.int32, (8, LANES), 0)
    lanes = row * SLOTS + lane % SLOTS
    for n, ref in enumerate((oo_ref, vo_ref, fo_ref)):
        for k in range(3):
            for c in range(4):
                line = jnp.broadcast_to(in_ref[3 * n + k, c : c + 1, :], (8, LANES))
                ref[c // 2, c % 2, k] = lane_take(line, lanes)[:, :SLOTS]
    hist_ref[...] = in_ref[9, :2, :STEPS]


def per_device(sizes, offsets, velocities, occupied):
    nx, ny, nz = sizes
    size_a, size_b = nz * 2, nx * (ny // 2)
    order = (0, 1, 4, 2, 3)
    block = jax.ShapeDtypeStruct((2, 2, 3, DEPTH, SLOTS), jnp.float32)
    whole = pl.BlockSpec(memory_space=pltpu.VMEM)
    dma = pltpu.SemaphoreType.DMA
    vmem = functools.partial(lambda *shape: pltpu.VMEM(shape, jnp.float32))
    lines = pl.pallas_call(
        functools.partial(kernel, sizes),
        out_shape=pltpu.VMEM((10, 8, LANES), jnp.float32),
        in_specs=[pl.BlockSpec(memory_space=pl.ANY)] * 3,
        out_specs=whole,
        scratch_shapes=[
            vmem(2, 2, 3, DEPTH, SLOTS), vmem(2, 2, 3, DEPTH, SLOTS), pltpu.VMEM((2, 2, DEPTH, SLOTS), jnp.int32), dma((3,)),
            vmem(ROUNDS, 4, 4, 2, 4, LANES),
            vmem(ROUNDS, 2, 2, 2, 1, LANES),
            vmem(ROUNDS, 2, 4, 4, 1, LANES),
            vmem(STEPS, size_a, 1, LANES),
            vmem(STEPS, size_b, 1, LANES),
            vmem(16, 2, 4, LANES),
            vmem(16, 3, 3, 2, 8, LANES),
            vmem(5, 4, 8, LANES),
            vmem(16, 8, LANES),
            vmem(3, 3, 8, LANES),
            vmem(4, 8, LANES),
            dma((ROUNDS,)), dma((ROUNDS,)), dma((ROUNDS,)), dma((ROUNDS,)),
            dma((STEPS,)), dma((STEPS,)), dma((STEPS,)), dma((STEPS,)),
        ],
        compiler_params=pltpu.CompilerParams(collective_id=0, has_side_effects=True),
        name="window",
    )(offsets.transpose(order), velocities.transpose(order), occupied)
    position, velocity, force, history = pl.pallas_call(
        unfold,
        out_shape=(block, block, block, jax.ShapeDtypeStruct((2, STEPS), jnp.float32)),
        in_specs=[whole],
        out_specs=(whole,) * 4,
        name="unfold",
    )(pltpu.with_memory_space_constraint(lines, pltpu.VMEM))
    back = (0, 1, 3, 4, 2)
    return (position.transpose(back), velocity.transpose(back), force.transpose(back), history.T)


def solution(mesh):
    sizes = tuple(mesh.shape[a] for a in ("gx", "gy", "gz"))
    cells = P("gx", "gy", "gz", None, None)
    return jax.shard_map(
        functools.partial(per_device, sizes),
        mesh=mesh,
        in_specs=(cells, cells, P("gx", "gy", "gz", None)),
        out_specs=(cells, cells, cells, P()),
        check_vma=False,
    )
```

```python
import functools
import itertools

import jax
import jax.numpy as jnp
from jax import lax
from jax.experimental import pallas as pl
from jax.experimental.pallas import tpu as pltpu
from jax.sharding import PartitionSpec as P

STEPS = 4
ROUNDS = STEPS + 1
CUTOFF = 2.5
CELL_SIDE = 2.6
TIME_STEP = 0.005
BATH_STRENGTH = 0.25
GOAL_WARMTH = 0.8
FORCE_EDGE = 24.0 * (2.0 * CUTOFF ** (-13) - CUTOFF ** (-7))
ENERGY_EDGE = 4.0 * (CUTOFF ** (-12) - CUTOFF ** (-6))
ENERGY_SHIFT = -ENERGY_EDGE - CUTOFF * FORCE_EDGE
UNIT = 2.0 ** (1.0 / 6.0)
SIDE = CELL_SIDE / UNIT
EDGE = FORCE_EDGE * UNIT / 12.0
REACH = (CUTOFF / UNIT) ** 2
FAR = 64.0
MESH = pl.DeviceIdType.MESH
LANES = 128
SLOTS = 16
DEPTH = 8

SIDES = {0: (pl.ds(0, 2), pl.ds(1, 2)), 1: (pl.ds(1, 1), pl.ds(0, 1)), -1: (pl.ds(0, 1), pl.ds(3, 1))}
NEIGHBOURS = sorted(
    (d for d in itertools.product((-1, 0, 1), repeat=3) if d != (0, 0, 0)),
    key=lambda d: -(2 * abs(d[0]) + 2 * abs(d[1]) + abs(d[2])),
)


def lane_take(x, lanes):
    return jnp.take_along_axis(x, lanes, axis=1, mode="promise_in_bounds")


def kernel(
    sizes, o_hbm, v_hbm, w_hbm, out_ref, o_ref, v_ref, w_ref, in_sem,
    buf, zsrc, zbuf, red_a, red_b, tally_a, tally_b, tally, lines, expand, acc, state, shifted, strip,
    halo_recv, halo_send, z_recv, z_send, a_recv, a_send, b_recv, b_send, tally_sems,
):
    nx, ny, nz = sizes
    gx, gy, gz = (lax.axis_index(a) for a in ("gx", "gy", "gz"))
    high, core = gy // 2, gy % 2
    n_high = ny // 2

    def at(dx, dy, dz):
        return (lax.rem(gx + dx + nx, nx), lax.rem(gy + dy + ny, ny), lax.rem(gz + dz + nz, nz))

    group_a = [
        (gx, high * 2 + lax.rem(core + dc, 2), lax.rem(gz + dz, nz))
        for dz in range(nz) for dc in range(2) if (dz, dc) != (0, 0)
    ]
    me_a = gz * 2 + core
    group_b = [
        (lax.rem(gx + dx, nx), lax.rem(high + dh, n_high) * 2 + core, gz)
        for dx in range(nx) for dh in range(n_high) if (dx, dh) != (0, 0)
    ]
    me_b = gx * n_high + high
    size_a, size_b = nz * 2, nx * n_high

    barrier = pltpu.get_barrier_semaphore()
    peers = [at(*d) for d in NEIGHBOURS] + group_a + group_b
    for peer in peers:
        pl.semaphore_signal(barrier, inc=1, device_id=peer, device_id_type=MESH)

    fetches = [
        pltpu.make_async_copy(src, dst, in_sem.at[n])
        for n, (src, dst) in enumerate(((o_hbm, o_ref), (v_hbm, v_ref), (w_hbm, w_ref)))
    ]
    for fetch in fetches:
        fetch.start()

    lane = lax.broadcasted_iota(jnp.int32, (8, LANES), 1)
    row = lax.broadcasted_iota(jnp.int32, (8, LANES), 0)
    slot, cell = lane % SLOTS, lane // SLOTS
    lane1 = lane[:1]

    def flatten(n, block):
        expand[n // 18, n // 6 % 3, n // 2 % 3, n % 2, :, :SLOTS] = block
        spread = lane_take(expand[n // 18, n // 6 % 3, n // 2 % 3, n % 2], slot)
        return jnp.sum(jnp.where(cell == row, spread, 0.0), axis=0, keepdims=True)

    for k in range(16):
        state[k] = jnp.zeros((8, LANES), jnp.float32)
    POS, VEL, FORCE, BASE, TERM, WEIGHT = 0, 3, 6, 9, 12, 15
    for fetch in fetches:
        fetch.wait()
    for c in range(4):
        cx, cy = c // 2, c % 2
        state[WEIGHT, c : c + 1, :] = flatten(7 * c, w_ref[cx, cy].astype(jnp.float32))
        for k in range(3):
            state[BASE + k, c : c + 1, :] = flatten(7 * c + 1 + k, o_ref[cx, cy, k])
            state[VEL + k, c : c + 1, :] = flatten(7 * c + 4 + k, v_ref[cx, cy, k])
    for k in range(3):
        state[VEL + k] = state[VEL + k] * state[WEIGHT]
    acc[...] = jnp.zeros_like(acc)
    for r in range(ROUNDS):
        for cx in range(2):
            for cy in range(2):
                buf[r, 1 + cx, 1 + cy] = jnp.zeros((2, 4, LANES), jnp.float32)

    def ship(r):
        here = state[WEIGHT] > 0.5
        base = [jnp.where(here, state[BASE + k], FAR) for k in range(3)]
        term = [state[TERM + k] for k in range(3)]
        for c in range(4):
            for k in range(3):
                buf[r, 1 + c // 2, 1 + c % 2, 0, k : k + 1, :] = base[k][c : c + 1]
                buf[r, 1 + c // 2, 1 + c % 2, 1, k : k + 1, :] = term[k][c : c + 1]
        for end in range(2):
            pick = slot + end * (LANES - SLOTS)
            packed = jnp.zeros((8, LANES), jnp.float32)
            for k in range(3):
                place = (2 * k + (DEPTH - 1) * end) % DEPTH
                packed = jnp.where(cell == place, lane_take(base[k], pick), packed)
                packed = jnp.where(cell == (place + 1) % DEPTH, lane_take(term[k], pick), packed)
            for c in range(4):
                zsrc[r, end, c // 2, c % 2] = packed[c : c + 1]
        for dx, dy, dz in NEIGHBOURS:
            (from_x, to_x), (from_y, to_y) = SIDES[dx], SIDES[dy]
            if dz == 0:
                own_x, own_y = pl.ds(from_x.start + 1, from_x.size), pl.ds(from_y.start + 1, from_y.size)
                pltpu.make_async_remote_copy(
                    src_ref=buf.at[r, own_x, own_y], dst_ref=buf.at[r, to_x, to_y],
                    send_sem=halo_send.at[r], recv_sem=halo_recv.at[r],
                    device_id=at(dx, dy, dz), device_id_type=MESH,
                ).start()
            else:
                end = 0 if dz < 0 else 1
                pltpu.make_async_remote_copy(
                    src_ref=zsrc.at[r, end, from_x, from_y], dst_ref=zbuf.at[r, end, to_x, to_y],
                    send_sem=z_send.at[r], recv_sem=z_recv.at[r],
                    device_id=at(dx, dy, dz), device_id_type=MESH,
                ).start()

    def all_of(ref, sem):
        pltpu.make_async_copy(ref, ref, sem).wait()

    def share(stage, me, group, send_sem, recv_sem, k, value):
        stage[k, me] = value
        for peer in group:
            pltpu.make_async_remote_copy(
                src_ref=stage.at[k, me], dst_ref=stage.at[k, me],
                send_sem=send_sem, recv_sem=recv_sem,
                device_id=peer, device_id_type=MESH,
            ).start()

    def collect(stage, size, recv_sem, k):
        all_of(stage.at[k, pl.ds(0, size - 1)], recv_sem)
        return jnp.sum(stage[k], axis=0)

    def half_sum(value, width):
        while width < LANES:
            value = value + pltpu.roll(value, width, 1)
            width *= 2
        return value

    count = jnp.sum(state[WEIGHT], axis=0, keepdims=True)

    pl.semaphore_wait(barrier, len(peers))
    ship(0)
    share(tally_a, me_a, group_a, tally_sems.at[0], tally_sems.at[1], 0, count)

    def one_round(r, stretch):
        wide = jnp.broadcast_to(stretch, (8, LANES))
        half_step = jnp.where(r == 0, 0.0, 0.5 * TIME_STEP)
        here = state[WEIGHT] > 0.5
        position, velocity = [], []
        for k in range(3):
            position.append(state[BASE + k] + wide * state[TERM + k])
            velocity.append(wide * state[VEL + k] + (0.5 * TIME_STEP) * state[FORCE + k])
            state[POS + k] = position[k]
            for dz in (-1, 0, 1):
                moved = position[k] * (1.0 / UNIT)
                moved = pltpu.roll(moved, (SLOTS * dz) % LANES, 1) if dz else moved
                shifted[dz + 1, k] = moved - SIDE * dz if k == 2 else moved

        all_of(buf.at[r, pl.ds(0, 3)], halo_recv.at[r])
        all_of(zbuf.at[r], z_recv.at[r])

        narrow = wide[:1]
        for x in range(4):
            for y in range(4):
                lines[x * 4 + y, 0] = (buf[r, x, y, 0] + wide[:4] * buf[r, x, y, 1]) * (1.0 / UNIT)
                ends = [zbuf[r, e, x, y] for e in range(2)]
                ends = [e + narrow * pltpu.roll(e, LANES - SLOTS, 1) for e in ends]
                ends = jnp.where(cell[:1] % 2 == 0, ends[0], ends[1]) * (1.0 / UNIT)
                for k in range(3):
                    turned = pltpu.roll(ends, LANES - 2 * SLOTS * k, 1) if k else ends
                    lines[x * 4 + y, 1, k : k + 1, :] = turned
        for h in range(2):
            spread_lanes = cell * SLOTS + row + 8 * h
            for n in range(16):
                for k in range(3):
                    level, ghost = (
                        lane_take(jnp.broadcast_to(lines[n, e, k : k + 1, :], (8, LANES)), spread_lanes)
                        for e in range(2)
                    )
                    expand[n, 0, k, h] = jnp.where(cell == DEPTH - 1, ghost, level)
                    expand[n, 1, k, h] = level
                    expand[n, 2, k, h] = jnp.where(cell == 0, ghost, level)

        def one_column(c, carry):
            base = (c // 2) * 4 + c % 2
            total = [None] * 4
            for dz in (-1, 0, 1):
                own = [jnp.broadcast_to(shifted[dz + 1, k, pl.ds(c, 1), :], (8, LANES)) for k in range(3)]
                part = [jnp.zeros((8, LANES), jnp.float32)] * 4
                distance = part[0]
                for dx in (-1, 0, 1):
                    own_x = own[0] - SIDE * dx
                    for dy in (-1, 0, 1):
                        own_y = own[1] - SIDE * dy
                        other = base + (dx + 1) * 4 + dy + 1
                        for h in range(2):
                            sx = expand[other, dz + 1, 0, h] - own_x
                            sy = expand[other, dz + 1, 1, h] - own_y
                            sz = expand[other, dz + 1, 2, h] - own[2]
                            squared = sx * sx + sy * sy + sz * sz
                            if (dx, dy, dz) == (0, 0, 0):
                                squared = jnp.where(slot == row + 8 * h, REACH, squared)
                            squared = jnp.minimum(squared, REACH)
                            inverse_root = lax.rsqrt(squared)
                            inverse = inverse_root * inverse_root
                            six = inverse * inverse * inverse
                            wall = six * (six - 1.0)
                            strength = wall * inverse - EDGE * inverse_root
                            part[0] = part[0] + strength * sx
                            part[1] = part[1] + strength * sy
                            part[2] = part[2] + strength * sz
                            part[3] = part[3] + (wall - six)
                            distance = distance + squared * inverse_root
                part[3] = part[3] + (12.0 * EDGE) * distance + 18.0 * ENERGY_SHIFT
                for k in range(4):
                    back = pltpu.roll(part[k], (-SLOTS * dz) % LANES, 1) if dz else part[k]
                    total[k] = back if total[k] is None else total[k] + back
            for k in range(4):
                acc[k, c] = total[k]
            return carry

        lax.fori_loop(0, 4, one_column, 0, unroll=4)

        sums = []
        for k in range(4):
            for c in range(4):
                strip[k, c : c + 1, :] = jnp.sum(acc[k, c], axis=0, keepdims=True)
        for k in range(4):
            sums.append(jnp.where(here & (row < 4), strip[k], 0.0))
        force, energy = [total * (-12.0 / UNIT) for total in sums[:3]], sums[3]
        vigor = jnp.zeros((8, LANES), jnp.float32)
        for k in range(3):
            velocity[k] = velocity[k] + half_step * force[k]
            vigor = vigor + velocity[k] * velocity[k]

        @pl.when(r > 0)
        def _():
            k_row = half_sum(jnp.sum(vigor, axis=0, keepdims=True), 64)
            u_row = half_sum(jnp.sum(energy, axis=0, keepdims=True), 64)
            value = jnp.where(lane1 < 64, k_row, u_row)
            share(red_a, me_a, group_a, a_send.at[r - 1], a_recv.at[r - 1], r - 1, value)

        for k in range(3):
            state[VEL + k] = velocity[k]
            state[FORCE + k] = force[k]
            state[BASE + k] = position[k] + (0.5 * TIME_STEP * TIME_STEP) * force[k]
            state[TERM + k] = TIME_STEP * velocity[k]

        @pl.when(r < STEPS)
        def _():
            ship(r + 1)

        @pl.when(r == 0)
        def _():
            value = collect(tally_a, size_a, tally_sems.at[1], 0)
            share(tally_b, me_b, group_b, tally_sems.at[2], tally_sems.at[3], 0, value)

        @pl.when(r == 1)
        def _():
            tally[...] = jnp.broadcast_to(collect(tally_b, size_b, tally_sems.at[3], 0), (8, LANES))

        def reduced():
            value = collect(red_a, size_a, a_recv.at[r - 1], r - 1)
            share(red_b, me_b, group_b, b_send.at[r - 1], b_recv.at[r - 1], r - 1, value)
            value = collect(red_b, size_b, b_recv.at[r - 1], r - 1)
            vigor_sum = 0.5 * jnp.sum(jnp.where(lane1 < 64, value, 0.0), axis=1, keepdims=True)
            body_tally = jnp.sum(tally[:1], axis=1, keepdims=True)
            potential = 0.5 * jnp.sum(jnp.where(lane1 >= 64, value, 0.0), axis=1, keepdims=True)
            warmth = 2.0 * vigor_sum / (3.0 * body_tally)
            new = jnp.sqrt(1.0 + BATH_STRENGTH * (GOAL_WARMTH / warmth - 1.0))
            slot_total = float(nx * ny * nz * 4 * DEPTH * SLOTS)
            record = jnp.where(row == 0, potential, new * new * vigor_sum) / slot_total
            acc[4, 0] = jnp.where(lane == r - 1, record, acc[4, 0])
            return new

        return lax.cond(r > 0, reduced, lambda: jnp.ones((1, 1), jnp.float32))

    stretch = lax.fori_loop(0, ROUNDS, one_round, jnp.ones((1, 1), jnp.float32))

    for k in range(3):
        out_ref[k] = state[POS + k]
        out_ref[3 + k] = stretch * state[VEL + k]
        out_ref[6 + k] = state[FORCE + k]
    out_ref[9] = acc[4, 0]

    def drain(r, carry):
        all_of(buf.at[r, pl.ds(0, 3)], halo_send.at[r])
        all_of(zbuf.at[r], z_send.at[r])
        return carry

    lax.fori_loop(0, ROUNDS, drain, 0)

    def drain_sums(k, carry):
        all_of(red_a.at[k, pl.ds(0, size_a - 1)], a_send.at[k])
        all_of(red_b.at[k, pl.ds(0, size_b - 1)], b_send.at[k])
        return carry

    lax.fori_loop(0, STEPS, drain_sums, 0)
    all_of(tally_a.at[0, pl.ds(0, size_a - 1)], tally_sems.at[0])
    all_of(tally_b.at[0, pl.ds(0, size_b - 1)], tally_sems.at[2])


def unfold(in_ref, oo_ref, vo_ref, fo_ref, hist_ref):
    lane = lax.broadcasted_iota(jnp.int32, (8, LANES), 1)
    row = lax.broadcasted_iota(jnp.int32, (8, LANES), 0)
    lanes = row * SLOTS + lane % SLOTS
    for n, ref in enumerate((oo_ref, vo_ref, fo_ref)):
        for k in range(3):
            for c in range(4):
                line = jnp.broadcast_to(in_ref[3 * n + k, c : c + 1, :], (8, LANES))
                ref[c // 2, c % 2, k] = lane_take(line, lanes)[:, :SLOTS]
    hist_ref[...] = in_ref[9, :2, :STEPS]


def per_device(sizes, offsets, velocities, occupied):
    nx, ny, nz = sizes
    size_a, size_b = nz * 2, nx * (ny // 2)
    order = (0, 1, 4, 2, 3)
    block = jax.ShapeDtypeStruct((2, 2, 3, DEPTH, SLOTS), jnp.float32)
    whole = pl.BlockSpec(memory_space=pltpu.VMEM)
    dma = pltpu.SemaphoreType.DMA
    vmem = functools.partial(lambda *shape: pltpu.VMEM(shape, jnp.float32))
    lines = pl.pallas_call(
        functools.partial(kernel, sizes),
        out_shape=pltpu.VMEM((10, 8, LANES), jnp.float32),
        in_specs=[pl.BlockSpec(memory_space=pl.ANY)] * 3,
        out_specs=whole,
        scratch_shapes=[
            vmem(2, 2, 3, DEPTH, SLOTS), vmem(2, 2, 3, DEPTH, SLOTS), pltpu.VMEM((2, 2, DEPTH, SLOTS), jnp.int32), dma((3,)),
            vmem(ROUNDS, 4, 4, 2, 4, LANES),
            vmem(ROUNDS, 2, 2, 2, 1, LANES),
            vmem(ROUNDS, 2, 4, 4, 1, LANES),
            vmem(STEPS, size_a, 1, LANES),
            vmem(STEPS, size_b, 1, LANES),
            vmem(1, size_a, 1, LANES),
            vmem(1, size_b, 1, LANES),
            vmem(8, LANES),
            vmem(16, 2, 4, LANES),
            vmem(16, 3, 3, 2, 8, LANES),
            vmem(5, 4, 8, LANES),
            vmem(16, 8, LANES),
            vmem(3, 3, 8, LANES),
            vmem(4, 8, LANES),
            dma((ROUNDS,)), dma((ROUNDS,)), dma((ROUNDS,)), dma((ROUNDS,)),
            dma((STEPS,)), dma((STEPS,)), dma((STEPS,)), dma((STEPS,)), dma((4,)),
        ],
        compiler_params=pltpu.CompilerParams(collective_id=0, has_side_effects=True),
        name="window",
    )(offsets.transpose(order), velocities.transpose(order), occupied)
    position, velocity, force, history = pl.pallas_call(
        unfold,
        out_shape=(block, block, block, jax.ShapeDtypeStruct((2, STEPS), jnp.float32)),
        in_specs=[whole],
        out_specs=(whole,) * 4,
        name="unfold",
    )(pltpu.with_memory_space_constraint(lines, pltpu.VMEM))
    back = (0, 1, 3, 4, 2)
    return (position.transpose(back), velocity.transpose(back), force.transpose(back), history.T)


def solution(mesh):
    sizes = tuple(mesh.shape[a] for a in ("gx", "gy", "gz"))
    cells = P("gx", "gy", "gz", None, None)
    return jax.shard_map(
        functools.partial(per_device, sizes),
        mesh=mesh,
        in_specs=(cells, cells, P("gx", "gy", "gz", None)),
        out_specs=(cells, cells, cells, P()),
        check_vma=False,
    )
```

```python
import functools
import itertools

import jax
import jax.numpy as jnp
from jax import lax
from jax.experimental import pallas as pl
from jax.experimental.pallas import tpu as pltpu
from jax.sharding import PartitionSpec as P

STEPS = 4
ROUNDS = STEPS + 1
CUTOFF = 2.5
CELL_SIDE = 2.6
TIME_STEP = 0.005
BATH_STRENGTH = 0.25
GOAL_WARMTH = 0.8
FORCE_EDGE = 24.0 * (2.0 * CUTOFF ** (-13) - CUTOFF ** (-7))
ENERGY_EDGE = 4.0 * (CUTOFF ** (-12) - CUTOFF ** (-6))
ENERGY_SHIFT = -ENERGY_EDGE - CUTOFF * FORCE_EDGE
UNIT = 2.0 ** (1.0 / 6.0)
SIDE = CELL_SIDE / UNIT
EDGE = FORCE_EDGE * UNIT / 12.0
REACH = (CUTOFF / UNIT) ** 2
FAR = 64.0
MESH = pl.DeviceIdType.MESH
LANES = 128
SLOTS = 16
DEPTH = 8

SIDES = {0: (pl.ds(0, 2), pl.ds(1, 2)), 1: (pl.ds(1, 1), pl.ds(0, 1)), -1: (pl.ds(0, 1), pl.ds(3, 1))}
NEIGHBOURS = sorted(
    (d for d in itertools.product((-1, 0, 1), repeat=3) if d != (0, 0, 0)),
    key=lambda d: -(2 * abs(d[0]) + 2 * abs(d[1]) + abs(d[2])),
)


def lane_take(x, lanes):
    return jnp.take_along_axis(x, lanes, axis=1, mode="promise_in_bounds")


def kernel(
    sizes, o_hbm, v_hbm, w_hbm, out_ref, o_ref, v_ref, w_ref, in_sem,
    buf, zsrc, zbuf, red_a, red_b, tally_a, tally_b, tally, lines, expand, acc, state, shifted, strip,
    halo_recv, halo_send, z_recv, z_send, a_recv, a_send, b_recv, b_send, tally_sems,
):
    nx, ny, nz = sizes
    gx, gy, gz = (lax.axis_index(a) for a in ("gx", "gy", "gz"))
    high, core = gy // 2, gy % 2
    n_high = ny // 2

    def at(dx, dy, dz):
        return (lax.rem(gx + dx + nx, nx), lax.rem(gy + dy + ny, ny), lax.rem(gz + dz + nz, nz))

    group_a = [
        (gx, high * 2 + lax.rem(core + dc, 2), lax.rem(gz + dz, nz))
        for dz in sorted(range(nz), key=lambda d: -min(d, nz - d)) for dc in (1, 0) if (dz, dc) != (0, 0)
    ]
    me_a = gz * 2 + core
    group_b = [
        (lax.rem(gx + dx, nx), lax.rem(high + dh, n_high) * 2 + core, gz)
        for dx in sorted(range(nx), key=lambda d: -min(d % 4, 4 - d % 4)) for dh in reversed(range(n_high)) if (dx, dh) != (0, 0)
    ]
    me_b = gx * n_high + high
    size_a, size_b = nz * 2, nx * n_high

    barrier = pltpu.get_barrier_semaphore()
    peers = [at(*d) for d in NEIGHBOURS] + group_a + group_b
    for peer in peers:
        pl.semaphore_signal(barrier, inc=1, device_id=peer, device_id_type=MESH)

    fetches = [
        pltpu.make_async_copy(src, dst, in_sem.at[n])
        for n, (src, dst) in enumerate(((o_hbm, o_ref), (v_hbm, v_ref), (w_hbm, w_ref)))
    ]
    for fetch in fetches:
        fetch.start()

    lane = lax.broadcasted_iota(jnp.int32, (8, LANES), 1)
    row = lax.broadcasted_iota(jnp.int32, (8, LANES), 0)
    slot, cell = lane % SLOTS, lane // SLOTS
    lane1 = lane[:1]

    def flatten(n, block):
        expand[n // 18, n // 6 % 3, n // 2 % 3, n % 2, :, :SLOTS] = block
        spread = lane_take(expand[n // 18, n // 6 % 3, n // 2 % 3, n % 2], slot)
        return jnp.sum(jnp.where(cell == row, spread, 0.0), axis=0, keepdims=True)

    for k in range(16):
        state[k] = jnp.zeros((8, LANES), jnp.float32)
    POS, VEL, FORCE, BASE, TERM, WEIGHT = 0, 3, 6, 9, 12, 15
    for fetch in fetches:
        fetch.wait()
    for c in range(4):
        cx, cy = c // 2, c % 2
        state[WEIGHT, c : c + 1, :] = flatten(7 * c, w_ref[cx, cy].astype(jnp.float32))
        for k in range(3):
            state[BASE + k, c : c + 1, :] = flatten(7 * c + 1 + k, o_ref[cx, cy, k])
            state[VEL + k, c : c + 1, :] = flatten(7 * c + 4 + k, v_ref[cx, cy, k])
    for k in range(3):
        state[VEL + k] = state[VEL + k] * state[WEIGHT]
    acc[...] = jnp.zeros_like(acc)
    for r in range(ROUNDS):
        for cx in range(2):
            for cy in range(2):
                buf[r, 1 + cx, 1 + cy] = jnp.zeros((2, 4, LANES), jnp.float32)

    def ship(r):
        here = state[WEIGHT] > 0.5
        base = [jnp.where(here, state[BASE + k], FAR) for k in range(3)]
        term = [state[TERM + k] for k in range(3)]
        for c in range(4):
            for k in range(3):
                buf[r, 1 + c // 2, 1 + c % 2, 0, k : k + 1, :] = base[k][c : c + 1]
                buf[r, 1 + c // 2, 1 + c % 2, 1, k : k + 1, :] = term[k][c : c + 1]
        for end in range(2):
            pick = slot + end * (LANES - SLOTS)
            packed = jnp.zeros((8, LANES), jnp.float32)
            for k in range(3):
                place = (2 * k + (DEPTH - 1) * end) % DEPTH
                packed = jnp.where(cell == place, lane_take(base[k], pick), packed)
                packed = jnp.where(cell == (place + 1) % DEPTH, lane_take(term[k], pick), packed)
            for c in range(4):
                zsrc[r, end, c // 2, c % 2] = packed[c : c + 1]
        for dx, dy, dz in NEIGHBOURS:
            (from_x, to_x), (from_y, to_y) = SIDES[dx], SIDES[dy]
            if dz == 0:
                own_x, own_y = pl.ds(from_x.start + 1, from_x.size), pl.ds(from_y.start + 1, from_y.size)
                pltpu.make_async_remote_copy(
                    src_ref=buf.at[r, own_x, own_y], dst_ref=buf.at[r, to_x, to_y],
                    send_sem=halo_send.at[r], recv_sem=halo_recv.at[r],
                    device_id=at(dx, dy, dz), device_id_type=MESH,
                ).start()
            else:
                end = 0 if dz < 0 else 1
                pltpu.make_async_remote_copy(
                    src_ref=zsrc.at[r, end, from_x, from_y], dst_ref=zbuf.at[r, end, to_x, to_y],
                    send_sem=z_send.at[r], recv_sem=z_recv.at[r],
                    device_id=at(dx, dy, dz), device_id_type=MESH,
                ).start()

    def all_of(ref, sem):
        pltpu.make_async_copy(ref, ref, sem).wait()

    def share(stage, me, group, send_sem, recv_sem, k, value):
        stage[k, me] = value
        for peer in group:
            pltpu.make_async_remote_copy(
                src_ref=stage.at[k, me], dst_ref=stage.at[k, me],
                send_sem=send_sem, recv_sem=recv_sem,
                device_id=peer, device_id_type=MESH,
            ).start()

    def collect(stage, size, recv_sem, k):
        all_of(stage.at[k, pl.ds(0, size - 1)], recv_sem)
        return jnp.sum(stage[k], axis=0)

    def half_sum(value, width):
        while width < LANES:
            value = value + pltpu.roll(value, width, 1)
            width *= 2
        return value

    count = jnp.sum(state[WEIGHT], axis=0, keepdims=True)

    pl.semaphore_wait(barrier, len(peers))
    ship(0)
    share(tally_a, me_a, group_a, tally_sems.at[0], tally_sems.at[1], 0, count)

    def one_round(r, stretch):
        wide = jnp.broadcast_to(stretch, (8, LANES))
        half_step = jnp.where(r == 0, 0.0, 0.5 * TIME_STEP)
        here = state[WEIGHT] > 0.5
        position, velocity = [], []
        for k in range(3):
            position.append(state[BASE + k] + wide * state[TERM + k])
            velocity.append(wide * state[VEL + k] + (0.5 * TIME_STEP) * state[FORCE + k])
            state[POS + k] = position[k]
            for dz in (-1, 0, 1):
                moved = position[k] * (1.0 / UNIT)
                moved = pltpu.roll(moved, (SLOTS * dz) % LANES, 1) if dz else moved
                shifted[dz + 1, k] = moved - SIDE * dz if k == 2 else moved

        all_of(buf.at[r, pl.ds(0, 3)], halo_recv.at[r])
        all_of(zbuf.at[r], z_recv.at[r])

        narrow = wide[:1]
        for x in range(4):
            for y in range(4):
                lines[x * 4 + y, 0] = (buf[r, x, y, 0] + wide[:4] * buf[r, x, y, 1]) * (1.0 / UNIT)
                ends = [zbuf[r, e, x, y] for e in range(2)]
                ends = [e + narrow * pltpu.roll(e, LANES - SLOTS, 1) for e in ends]
                ends = jnp.where(cell[:1] % 2 == 0, ends[0], ends[1]) * (1.0 / UNIT)
                for k in range(3):
                    turned = pltpu.roll(ends, LANES - 2 * SLOTS * k, 1) if k else ends
                    lines[x * 4 + y, 1, k : k + 1, :] = turned
        for h in range(2):
            spread_lanes = cell * SLOTS + row + 8 * h
            for n in range(16):
                for k in range(3):
                    level, ghost = (
                        lane_take(jnp.broadcast_to(lines[n, e, k : k + 1, :], (8, LANES)), spread_lanes)
                        for e in range(2)
                    )
                    expand[n, 0, k, h] = jnp.where(cell == DEPTH - 1, ghost, level)
                    expand[n, 1, k, h] = level
                    expand[n, 2, k, h] = jnp.where(cell == 0, ghost, level)

        def one_column(c, carry):
            base = (c // 2) * 4 + c % 2
            total = [None] * 4
            for dz in (-1, 0, 1):
                own = [jnp.broadcast_to(shifted[dz + 1, k, pl.ds(c, 1), :], (8, LANES)) for k in range(3)]
                part = [jnp.zeros((8, LANES), jnp.float32)] * 4
                distance = part[0]
                for dx in (-1, 0, 1):
                    own_x = own[0] - SIDE * dx
                    for dy in (-1, 0, 1):
                        own_y = own[1] - SIDE * dy
                        other = base + (dx + 1) * 4 + dy + 1
                        for h in range(2):
                            sx = expand[other, dz + 1, 0, h] - own_x
                            sy = expand[other, dz + 1, 1, h] - own_y
                            sz = expand[other, dz + 1, 2, h] - own[2]
                            squared = sx * sx + sy * sy + sz * sz
                            if (dx, dy, dz) == (0, 0, 0):
                                squared = jnp.where(slot == row + 8 * h, REACH, squared)
                            squared = jnp.minimum(squared, REACH)
                            inverse_root = lax.rsqrt(squared)
                            inverse = inverse_root * inverse_root
                            six = inverse * inverse * inverse
                            wall = six * (six - 1.0)
                            strength = wall * inverse - EDGE * inverse_root
                            part[0] = part[0] + strength * sx
                            part[1] = part[1] + strength * sy
                            part[2] = part[2] + strength * sz
                            part[3] = part[3] + (wall - six)
                            distance = distance + squared * inverse_root
                part[3] = part[3] + (12.0 * EDGE) * distance + 18.0 * ENERGY_SHIFT
                for k in range(4):
                    back = pltpu.roll(part[k], (-SLOTS * dz) % LANES, 1) if dz else part[k]
                    total[k] = back if total[k] is None else total[k] + back
            for k in range(4):
                acc[k, c] = total[k]
            return carry

        lax.fori_loop(0, 4, one_column, 0, unroll=4)

        sums = []
        for k in range(4):
            for c in range(4):
                strip[k, c : c + 1, :] = jnp.sum(acc[k, c], axis=0, keepdims=True)
        for k in range(4):
            sums.append(jnp.where(here & (row < 4), strip[k], 0.0))
        force, energy = [total * (-12.0 / UNIT) for total in sums[:3]], sums[3]
        vigor = jnp.zeros((8, LANES), jnp.float32)
        for k in range(3):
            velocity[k] = velocity[k] + half_step * force[k]
            vigor = vigor + velocity[k] * velocity[k]

        @pl.when(r > 0)
        def _():
            k_row = half_sum(jnp.sum(vigor, axis=0, keepdims=True), 64)
            u_row = half_sum(jnp.sum(energy, axis=0, keepdims=True), 64)
            value = jnp.where(lane1 < 64, k_row, u_row)
            share(red_a, me_a, group_a, a_send.at[r - 1], a_recv.at[r - 1], r - 1, value)

        for k in range(3):
            state[VEL + k] = velocity[k]
            state[FORCE + k] = force[k]
            state[BASE + k] = position[k] + (0.5 * TIME_STEP * TIME_STEP) * force[k]
            state[TERM + k] = TIME_STEP * velocity[k]

        @pl.when(r < STEPS)
        def _():
            ship(r + 1)

        @pl.when(r == 0)
        def _():
            value = collect(tally_a, size_a, tally_sems.at[1], 0)
            share(tally_b, me_b, group_b, tally_sems.at[2], tally_sems.at[3], 0, value)

        @pl.when(r == 1)
        def _():
            tally[...] = jnp.broadcast_to(collect(tally_b, size_b, tally_sems.at[3], 0), (8, LANES))

        def reduced():
            value = collect(red_a, size_a, a_recv.at[r - 1], r - 1)
            share(red_b, me_b, group_b, b_send.at[r - 1], b_recv.at[r - 1], r - 1, value)
            value = collect(red_b, size_b, b_recv.at[r - 1], r - 1)
            vigor_sum = 0.5 * jnp.sum(jnp.where(lane1 < 64, value, 0.0), axis=1, keepdims=True)
            body_tally = jnp.sum(tally[:1], axis=1, keepdims=True)
            potential = 0.5 * jnp.sum(jnp.where(lane1 >= 64, value, 0.0), axis=1, keepdims=True)
            warmth = 2.0 * vigor_sum / (3.0 * body_tally)
            new = jnp.sqrt(1.0 + BATH_STRENGTH * (GOAL_WARMTH / warmth - 1.0))
            slot_total = float(nx * ny * nz * 4 * DEPTH * SLOTS)
            record = jnp.where(row == 0, potential, new * new * vigor_sum) / slot_total
            acc[4, 0] = jnp.where(lane == r - 1, record, acc[4, 0])
            return new

        return lax.cond(r > 0, reduced, lambda: jnp.ones((1, 1), jnp.float32))

    stretch = lax.fori_loop(0, ROUNDS, one_round, jnp.ones((1, 1), jnp.float32))

    for k in range(3):
        out_ref[k] = state[POS + k]
        out_ref[3 + k] = stretch * state[VEL + k]
        out_ref[6 + k] = state[FORCE + k]
    out_ref[9] = acc[4, 0]

    def drain(r, carry):
        all_of(buf.at[r, pl.ds(0, 3)], halo_send.at[r])
        all_of(zbuf.at[r], z_send.at[r])
        return carry

    lax.fori_loop(0, ROUNDS, drain, 0)

    def drain_sums(k, carry):
        all_of(red_a.at[k, pl.ds(0, size_a - 1)], a_send.at[k])
        all_of(red_b.at[k, pl.ds(0, size_b - 1)], b_send.at[k])
        return carry

    lax.fori_loop(0, STEPS, drain_sums, 0)
    all_of(tally_a.at[0, pl.ds(0, size_a - 1)], tally_sems.at[0])
    all_of(tally_b.at[0, pl.ds(0, size_b - 1)], tally_sems.at[2])


def unfold(in_ref, oo_ref, vo_ref, fo_ref, hist_ref):
    lane = lax.broadcasted_iota(jnp.int32, (8, LANES), 1)
    row = lax.broadcasted_iota(jnp.int32, (8, LANES), 0)
    lanes = row * SLOTS + lane % SLOTS
    for n, ref in enumerate((oo_ref, vo_ref, fo_ref)):
        for k in range(3):
            for c in range(4):
                line = jnp.broadcast_to(in_ref[3 * n + k, c : c + 1, :], (8, LANES))
                ref[c // 2, c % 2, k] = lane_take(line, lanes)[:, :SLOTS]
    hist_ref[...] = in_ref[9, :2, :STEPS]


def per_device(sizes, offsets, velocities, occupied):
    nx, ny, nz = sizes
    size_a, size_b = nz * 2, nx * (ny // 2)
    order = (0, 1, 4, 2, 3)
    block = jax.ShapeDtypeStruct((2, 2, 3, DEPTH, SLOTS), jnp.float32)
    whole = pl.BlockSpec(memory_space=pltpu.VMEM)
    dma = pltpu.SemaphoreType.DMA
    vmem = functools.partial(lambda *shape: pltpu.VMEM(shape, jnp.float32))
    lines = pl.pallas_call(
        functools.partial(kernel, sizes),
        out_shape=pltpu.VMEM((10, 8, LANES), jnp.float32),
        in_specs=[pl.BlockSpec(memory_space=pl.ANY)] * 3,
        out_specs=whole,
        scratch_shapes=[
            vmem(2, 2, 3, DEPTH, SLOTS), vmem(2, 2, 3, DEPTH, SLOTS), pltpu.VMEM((2, 2, DEPTH, SLOTS), jnp.int32), dma((3,)),
            vmem(ROUNDS, 4, 4, 2, 4, LANES),
            vmem(ROUNDS, 2, 2, 2, 1, LANES),
            vmem(ROUNDS, 2, 4, 4, 1, LANES),
            vmem(STEPS, size_a, 1, LANES),
            vmem(STEPS, size_b, 1, LANES),
            vmem(1, size_a, 1, LANES),
            vmem(1, size_b, 1, LANES),
            vmem(8, LANES),
            vmem(16, 2, 4, LANES),
            vmem(16, 3, 3, 2, 8, LANES),
            vmem(5, 4, 8, LANES),
            vmem(16, 8, LANES),
            vmem(3, 3, 8, LANES),
            vmem(4, 8, LANES),
            dma((ROUNDS,)), dma((ROUNDS,)), dma((ROUNDS,)), dma((ROUNDS,)),
            dma((STEPS,)), dma((STEPS,)), dma((STEPS,)), dma((STEPS,)), dma((4,)),
        ],
        compiler_params=pltpu.CompilerParams(collective_id=0, has_side_effects=True),
        name="window",
    )(offsets.transpose(order), velocities.transpose(order), occupied)
    position, velocity, force, history = pl.pallas_call(
        unfold,
        out_shape=(block, block, block, jax.ShapeDtypeStruct((2, STEPS), jnp.float32)),
        in_specs=[whole],
        out_specs=(whole,) * 4,
        name="unfold",
    )(pltpu.with_memory_space_constraint(lines, pltpu.VMEM))
    back = (0, 1, 3, 4, 2)
    return (position.transpose(back), velocity.transpose(back), force.transpose(back), history.T)


def solution(mesh):
    sizes = tuple(mesh.shape[a] for a in ("gx", "gy", "gz"))
    cells = P("gx", "gy", "gz", None, None)
    return jax.shard_map(
        functools.partial(per_device, sizes),
        mesh=mesh,
        in_specs=(cells, cells, P("gx", "gy", "gz", None)),
        out_specs=(cells, cells, cells, P()),
        check_vma=False,
    )
```
